32 devices in a mesh: dp: 8 (over z, x), mp: 4 (over y, core).
Axes of the slice: x: 2, y: 2, z: 4, core: 2. Of those that a mesh axis runs over, the one named last changes fastest.
Arguments:
- gating_logits: bfloat16 [8, 3, 64, 7168], P('dp', None, None, 'mp'), may hold values from -6 to 6
- lifted_hidden_values: bfloat16 [8, 3, 64, 7168], P('dp', None, None, 'mp'), may hold values from -6 to 6
- loss_output_grad: bfloat16 [8, 3, 64, 2048], P('dp', None, None, 'mp'), may hold values from -160 to 160
- arrival_flags: int32 [8], P('dp'), may hold values from 0 to 1, as said below
- block_owner_map: int32 [8, 3], P('dp'), may hold values from 0 to 7, as said below
- decoder_multipliers: int32 [8, 3], P('dp'), may hold values from 1 to 4
- block_piece_number: int32 [8], replicated, may hold values from 1 to 2, as said below
Outputs:
- down_grad: float32 [2048, 7168], P('dp', 'mp')
The draws below stay inside these ranges and needn't reach their ends.
Inputs may be any that keep to these rules, and one draw needn't show every extreme that they name: `arrival_flags`: at least one replica survives. `block_owner_map`: row i lists the partitions (i + r + k) mod 8 for k < 3, with one r for all rows. `block_piece_number`: some partition has exactly 2 live tiles.
All inputs are finite; a program needn't handle non-finite values.
Results may differ from the reference program's by a relative error of at most 0.0042.
Values may be sent and summed in bfloat16 or wider, within the bound.
A program may use at most 128 MiB of HBM per device.

```python
import jax
import jax.numpy as jnp
from jax import lax

D = 2048
SLOTS = 3
TILE = 32
TILES = 2
TOK = 64
FF = 7168
N_DP = 8


def draw_arrival_flags(key, part):
    coin_flips = jax.random.randint(jax.random.fold_in(key, 11), (N_DP,), 0, 4)
    forced = jax.random.randint(jax.random.fold_in(key, 12), (), 0, N_DP)
    alive = jnp.where(coin_flips > 0, 1, 0)
    return jnp.where(jnp.arange(N_DP) == forced, 1, alive).astype(jnp.int32)


def draw_block_owner_map(key, part):
    rotation = jax.random.randint(jax.random.fold_in(key, 21), (), 0, N_DP)
    rows_idx = jnp.arange(N_DP, dtype=jnp.int32)[:, None]
    slot_idx = jnp.arange(SLOTS, dtype=jnp.int32)[None, :]
    return ((rows_idx + rotation + slot_idx) % N_DP).astype(jnp.int32)


def draw_block_piece_number(key, part):
    part_ids = jnp.arange(N_DP, dtype=jnp.int32)
    baseline = 1 + part_ids * (TILES - 1) // max(N_DP - 1, 1)
    jitter = jax.random.randint(jax.random.fold_in(key, 31), (N_DP,), 0, 2)
    return jnp.minimum(baseline + jitter, TILES).astype(jnp.int32)


def plant(array, own_key, low, high):
    shape = array.shape
    spot = [jax.random.randint(jax.random.fold_in(own_key, axis), (), 0, shape[axis]) for axis in range(len(shape))]
    array = array.at[tuple(spot)].set(low)
    longest = shape.index(max(shape))
    spot[longest] = (spot[longest] + 1) % shape[longest]
    return array.at[tuple(spot)].set(high)


def strengthened(entries, key, source, target, blocks, factor):
    owner, partner = [(jnp.arange(entries.shape[dim]) // (entries.shape[dim] // blocks)).reshape([-1 if axis == dim else 1 for axis in range(entries.ndim)]) for dim in (source, target)]
    chosen = jax.random.permutation(key, blocks)[partner]
    strong = (owner == chosen) | (owner == (partner + blocks // 2) % blocks)
    return jnp.where(strong, factor * entries, entries)


def shard_levels(own_key, extent, cuts, smallest, top_value):
    gain, own = 1.0, jax.random.fold_in(own_key, 6)
    for axis_at, blocks in cuts:
        steps = jnp.exp(jax.random.uniform(jax.random.fold_in(own, axis_at), (blocks,), jnp.float32, smallest / len(cuts), top_value / len(cuts)))
        gain = gain * jnp.repeat(steps, extent[axis_at] // blocks).reshape([-1 if axis == axis_at else 1 for axis in range(len(extent))])
    return gain


def normal_values(rng, dims, deviation, reach, cuts=(), held_as=jnp.bfloat16):
    result = deviation * jax.random.normal(rng, dims, jnp.float32)
    if cuts:
        result = result * shard_levels(rng, dims, cuts, -0.22, 0.18)
    return jnp.clip(result, -reach, reach).astype(held_as)


def noise_with(own_key, shape, scale, limit, cuts, heavy, held_as=jnp.bfloat16):
    result = scale * jax.random.normal(own_key, shape, jnp.float32)
    if cuts:
        result = result * shard_levels(own_key, shape, cuts, -0.22, 0.18)
    return jnp.clip(strengthened(result, jax.random.fold_in(own_key, 3), *heavy), -limit, limit).astype(held_as)


def setup_inputs(seed: int = 0) -> dict:
    key_of = jax.random.split(jax.random.key(seed), 8)
    return {
        "gating_logits": normal_values(key_of[0], (N_DP, SLOTS, TOK, FF), 1.0, 6.0, ((0, 8), (3, 4))),
        "lifted_hidden_values": normal_values(key_of[1], (N_DP, SLOTS, TOK, FF), 1.0, 6.0, ((0, 8), (3, 4))),
        "loss_output_grad": noise_with(key_of[2], (N_DP, SLOTS, TOK, D), ((N_DP * SLOTS * TOK) ** 0.5 / 2), 160.0, ((0, 8), (3, 4)), (0, 3, 8, 2.0)),
        "arrival_flags": draw_arrival_flags(jax.random.fold_in(key_of[7], 71), 0),
        "block_owner_map": draw_block_owner_map(jax.random.fold_in(key_of[7], 71), 0),
        "decoder_multipliers": plant(jax.random.randint(key_of[5], (N_DP, SLOTS), 1, 5), jax.random.fold_in(key_of[5], 1), 1, 4).astype(jnp.int32),
        "block_piece_number": draw_block_piece_number(jax.random.fold_in(key_of[7], 71), 0),
    }


def reference(gating_logits, lifted_hidden_values, loss_output_grad, arrival_flags, block_owner_map, decoder_multipliers, block_piece_number):
    part_ids = jnp.arange(N_DP, dtype=jnp.int32)
    slot_tiles = jnp.sum(jnp.where(block_owner_map[:, :, None] == part_ids[None, None, :], block_piece_number[None, None, :], 0), axis=2)
    live_rows = slot_tiles * TILE
    live_mask = jnp.arange(TOK, dtype=jnp.int32)[None, None, :] < live_rows[:, :, None]
    down_kernel_array = arrival_flags[:, None].astype(jnp.float32) * decoder_multipliers.astype(jnp.float32)
    total_tokens = jnp.sum(down_kernel_array * live_rows.astype(jnp.float32))

    def accumulate(running_total, current_inputs):
        gate_now, current_up_projection, cot_now, weight_now, live_now = current_inputs
        hidden = (jax.nn.silu(gate_now.astype(jnp.float32)) * current_up_projection.astype(jnp.float32) * live_now[:, :, None].astype(jnp.float32)).astype(jnp.bfloat16)
        scaled = hidden.astype(jnp.float32) * weight_now[:, None, None]
        contrib = jnp.einsum("ktd,ktf->df", cot_now.astype(jnp.float32), scaled, precision=lax.Precision.HIGHEST)
        return running_total + contrib, None

    start_sum = jnp.zeros((D, FF), jnp.float32)
    coded, _ = lax.scan(accumulate, start_sum, (gating_logits, lifted_hidden_values, loss_output_grad, down_kernel_array, live_mask))
    return coded / total_tokens
```

```python
import functools

import jax
import jax.numpy as jnp
from jax import lax
from jax.experimental import pallas as pl
from jax.experimental.pallas import tpu as pltpu
from jax.sharding import PartitionSpec as P

TILE = 32
CHUNK = 256
SHARED = (3, 5)
AHEAD = 3
EARLY = 2
STAGES = (1, 2, 2)
LAG = 2


def kernel(
    sizes,
    flags_ref,
    owner_ref,
    mult_ref,
    pieces_ref,
    gate_hbm,
    lift_hbm,
    cot_hbm,
    out_ref,
    gate_in,
    lift_in,
    cot_ref,
    quarters,
    hid,
    cot_all,
    cot_t,
    part,
    arrived,
    tok_mine,
    tok_g,
    tok_sum,
    tok_r,
    cot_x,
    cot_own,
    cot_e,
    mine_e,
    give_e,
    take_e,
    sum_e,
    from_e,
    load_c,
    load_g,
    load_l,
    send_1,
    recv_1,
    send_2,
    recv_2,
    send_3,
    recv_3,
    send_up,
    send_dn,
    recv_h,
    send_p,
    recv_p,
    send_tg,
    recv_tg,
    send_tr,
    recv_tr,
    send_x,
    recv_x,
    send_y,
    recv_y,
    send_e,
    recv_e,
    send_f,
    recv_f,
    send_r,
):
    G, R, M, slots, toks, chunks, rows, shared = sizes
    n = slots * toks
    d = lax.axis_index("dp")
    m = lax.axis_index("mp")
    g = d // R
    r = d % R
    quarter = n // M
    pair = M == 4
    m1 = m + 1 - 2 * (m % 2)
    m2 = m + 2 - 4 * (m // 2)
    m3 = m1 + 2 - 4 * (m1 // 2)

    at_edge = jnp.logical_or(g == 0, g == G - 1)
    is_dn = g == 1
    helper = jnp.logical_or(g == 1, g == G - 2)
    base = jnp.where(is_dn, 1, 0)
    edge = jnp.where(is_dn, 0, G - 1)

    def dev(g_to, r_to, m_to):
        return {"dp": g_to * R + r_to, "mp": m_to}

    def remote(src, dst, s, q, where):
        return pltpu.make_async_remote_copy(
            src_ref=src,
            dst_ref=dst,
            send_sem=s,
            recv_sem=q,
            device_id=where,
            device_id_type=pl.DeviceIdType.MESH,
        )

    def spread_copy(off):
        m_to = (m + off) % M
        return remote(
            cot_ref.at[pl.ds(pl.multiple_of(m_to * quarter, quarter), quarter)],
            quarters.at[m],
            send_1.at[off],
            recv_1.at[m],
            dev(g, r, m_to),
        )

    def spread_in(off):
        m_from = (m + off) % M
        return remote(
            quarters.at[m_from],
            quarters.at[m_from],
            send_1.at[off],
            recv_1.at[m_from],
            dev(g, r, m_from),
        )

    def cross_copy(g_to):
        return remote(
            quarters.at[g_to], cot_all.at[m, g], send_2.at[g_to], recv_2.at[g], dev(g_to, r, m)
        )

    def cross_in(g_from):
        return remote(
            quarters.at[g],
            cot_all.at[m, g_from],
            send_2.at[g_from],
            recv_2.at[g_from],
            dev(g_from, r, m),
        )

    def extra_copy(g_to, block, s):
        return remote(
            quarters.at[block], cot_x.at[m, g], send_x.at[s], recv_x.at[g], dev(g_to, r, m)
        )

    def extra_relay(g_from):
        return remote(
            cot_x.at[m, g_from],
            cot_all.at[m, g_from],
            send_r.at[g_from],
            recv_2.at[g_from],
            dev(edge, r, m),
        )

    def extra_in(g_from):
        return remote(
            quarters.at[0], cot_x.at[m, g_from], send_x.at[0], recv_x.at[g_from], dev(g_from, r, m)
        )

    def share(src, buf, origin, i, way, to, sends, recvs):
        return remote(
            src, buf.at[origin, i], sends.at[way, i], recvs.at[origin, i], dev(g, r, to)
        )

    peers = [m1, m2] if pair else [(m + off) % M for off in range(1, M)]

    def share_out(buf, src, i, sends, recvs):
        for way, to in enumerate(peers):
            share(src, buf, m, i, way, to, sends, recvs).start()

    def relay(buf, i, sends, recvs):
        if pair:
            share(buf.at[m2, i], buf, m2, i, 2, m1, sends, recvs).wait_recv()
            share(buf.at[m2, i], buf, m2, i, 2, m1, sends, recvs).start()

    def share_end(buf, i, sends, recvs):
        for o in [m1, m3] if pair else peers:
            share(buf.at[o, i], buf, o, i, 0, m1, sends, recvs).wait_recv()

    def share_drain(buf, i, sends, recvs):
        for way, to in enumerate(peers):
            share(buf.at[m, i], buf, m, i, way, to, sends, recvs).wait_send()
        if pair:
            share(buf.at[m2, i], buf, m2, i, 2, m1, sends, recvs).wait_send()

    def others(body):
        for k in range(1, G):

            @pl.when(g >= k)
            def _():
                body(g - k)

            @pl.when(g + k < G)
            def _():
                body(g + k)

    def extras(body):
        @pl.when(helper)
        def _():
            for k in range(1, G - 1):
                body(jnp.where(is_dn, g + k, g - k))

    def load(src, dst, c, sem):
        return pltpu.make_async_copy(
            src.at[:, pl.ds(c * CHUNK, CHUNK)], dst.at[c], sem.at[c]
        )

    def hop(c, origin, to, sems):
        return remote(
            hid.at[c, origin],
            hid.at[c, origin],
            sems.at[c, origin],
            recv_h.at[c, origin],
            dev(to, r, m),
        )

    up, down = (g + 1) % G, (g + G - 1) % G

    def goes_up(c):
        return g < (G - 2 if c in shared else G - 1)

    def goes_down(c):
        return g > (1 if c in shared else 0)

    def pass_on(c, origin, has_next, to, sems):
        hop(c, origin, to, sems).wait_recv()

        @pl.when(has_next)
        def _():
            hop(c, origin, to, sems).start()

    def receive(c, k):
        from_left = g >= k
        from_right = g + k < G
        if c in shared:
            from_left = jnp.logical_and(from_left, g < G - 1)
            from_right = jnp.logical_and(from_right, g > 0)

        @pl.when(from_left)
        def _():
            pass_on(c, (g + G - k) % G, goes_up(c), up, send_up)

        @pl.when(from_right)
        def _():
            pass_on(c, (g + k) % G, goes_down(c), down, send_dn)

    def part_copy(c, off):
        r_to = (r + off) % R
        return remote(
            part.at[c, r_to], arrived.at[c, r], send_p.at[c, off], recv_p.at[c, r], dev(g, r_to, m)
        )

    def part_in(c, off):
        r_from = (r + off) % R
        return remote(
            part.at[c, r_from],
            arrived.at[c, r_from],
            send_p.at[c, off],
            recv_p.at[c, r_from],
            dev(g, r_from, m),
        )

    def swap_e(b):
        return remote(
            give_e.at[b], take_e.at[b], send_e.at[b], recv_e.at[b], dev(g, (r + 1) % R, m)
        )

    def final_e(b, to):
        return remote(sum_e.at[b], from_e.at[b], send_f.at[b], recv_f.at[b], dev(to, r, m))

    def tok_copy(off):
        return remote(
            tok_mine, tok_g.at[g], send_tg.at[off], recv_tg.at[g], dev((g + off) % G, r, m)
        )

    def tok_in(off):
        g_from = (g + off) % G
        return remote(
            tok_mine, tok_g.at[g_from], send_tg.at[off], recv_tg.at[g_from], dev(g_from, r, m)
        )

    def sum_copy(off):
        return remote(
            tok_sum, tok_r.at[r], send_tr.at[off], recv_tr.at[r], dev(g, (r + off) % R, m)
        )

    def sum_in(off):
        r_from = (r + off) % R
        return remote(
            tok_sum, tok_r.at[r_from], send_tr.at[off], recv_tr.at[r_from], dev(g, r_from, m)
        )

    def over_r(body):
        def step(off, carry):
            body(off)
            return carry

        lax.fori_loop(1, R, step, 0)

    load_cot = pltpu.make_async_copy(cot_hbm, cot_ref, load_c)
    load_cot.start()
    for c in range(chunks):
        load(gate_hbm, gate_in, c, load_g).start()
        load(lift_hbm, lift_in, c, load_l).start()

    barrier = pltpu.get_barrier_semaphore()

    def greet(where):
        pl.semaphore_signal(
            barrier, inc=1, device_id=where, device_id_type=pl.DeviceIdType.MESH
        )

    for off in range(1, M):
        greet(dev(g, r, (m + off) % M))
    for off in range(1, G):
        greet(dev((g + off) % G, r, m))
    over_r(lambda off: greet(dev(g, (r + off) % R, m)))

    flag = flags_ref[0].astype(jnp.float32)
    scales = []
    token_sum = jnp.float32(0)
    row = lax.broadcasted_iota(jnp.int32, (toks, CHUNK), 0)
    for k in range(slots):
        live = pieces_ref[owner_ref[0, k]] * TILE
        weight = flag * mult_ref[0, k].astype(jnp.float32)
        scales.append(jnp.where(row < live, weight, 0.0))
        token_sum = token_sum + weight * live.astype(jnp.float32)
    tok_mine[...] = jnp.full(tok_mine.shape, token_sum, jnp.float32)

    def make_hidden(c):
        load(gate_hbm, gate_in, c, load_g).wait()
        load(lift_hbm, lift_in, c, load_l).wait()
        for k in range(slots):
            rk = pl.ds(k * toks, toks)
            v = gate_in[c, rk, :].astype(jnp.float32)
            u = lift_in[c, rk, :].astype(jnp.float32)
            h = v / (1.0 + jnp.exp(-v)) * u * scales[k]
            hid[c, g, rk, :] = h.astype(jnp.bfloat16)

    def send_hidden(c):
        @pl.when(goes_up(c))
        def _():
            hop(c, g, up, send_up).start()

        @pl.when(goes_down(c))
        def _():
            hop(c, g, down, send_dn).start()

    load_cot.wait()
    quarters[m] = cot_ref[pl.ds(pl.multiple_of(m * quarter, quarter), quarter), :]
    make_hidden(0)
    pl.semaphore_wait(barrier, M - 1 + G - 1 + R - 1)

    for off in range(1, M):
        spread_copy(off).start()
    send_hidden(0)
    for off in range(1, G):
        tok_copy(off).start()
    for c in range(1, EARLY):
        make_hidden(c)
        send_hidden(c)
    for off in range(1, M):
        spread_in(off).wait_recv()
    def direct(i, body):
        if not shared:
            body(cross_copy(i))
            return
        by_hand = jnp.logical_or(
            jnp.logical_and(i == G - 1, g < G - 2), jnp.logical_and(i == 0, g > 1)
        )

        @pl.when(jnp.logical_not(by_hand))
        def _():
            body(cross_copy(i))

    others(lambda i: direct(i, lambda copy: copy.start()))
    if shared:

        @pl.when(g < G - 2)
        def _():
            extra_copy(G - 2, G - 1, 0).start()

        @pl.when(g > 1)
        def _():
            extra_copy(1, 0, 1).start()

    share_out(cot_all, quarters.at[g], g, send_3, recv_3)
    cot_all[m, g] = quarters[g]
    if shared:

        @pl.when(helper)
        def _():
            share_out(cot_x, quarters.at[edge], g, send_y, recv_y)
            cot_x[m, g] = quarters[edge]

    for c in range(EARLY, AHEAD):
        make_hidden(c)
        send_hidden(c)

    def share_more():
        if shared:

            def more(i):
                extra_in(i).wait_recv()
                extra_relay(i).start()
                share_out(cot_x, cot_x.at[m, i], i, send_y, recv_y)

            extras(more)

        def one(i):
            cross_in(i).wait_recv()
            share_out(cot_all, cot_all.at[m, i], i, send_3, recv_3)

        others(one)

    def relay_all():
        relay(cot_all, g, send_3, recv_3)
        others(lambda i: relay(cot_all, i, send_3, recv_3))
        if shared:

            @pl.when(helper)
            def _():
                relay(cot_x, g, send_y, recv_y)

            extras(lambda i: relay(cot_x, i, send_y, recv_y))

    def turn():
        for i in range(G):
            share_end(cot_all, i, send_3, recv_3)
            block = jnp.concatenate([cot_all[j, i] for j in range(M)], axis=0)
            cot_t[:, pl.ds(i * n, n)] = block.T
        if shared:

            @pl.when(at_edge)
            def _():
                block = jnp.concatenate([cot_all[j, g] for j in range(M)], axis=0)
                cot_own[...] = block.T

            @pl.when(helper)
            def _():
                for i in range(G - 1):
                    share_end(cot_x, base + i, send_y, recv_y)
                    block = jnp.concatenate([cot_x[j, base + i] for j in range(M)], axis=0)
                    cot_e[:, pl.ds(i * n, n)] = block.T

    def product(left, block):
        return jnp.dot(left, block, preferred_element_type=jnp.float32)

    def strip(ref, which):
        return ref[pl.ds(pl.multiple_of(which * rows, rows), rows), :]

    def main(c, left_ref, block):
        def other(off):
            r_to = (r + off) % R
            part[c, r_to] = product(strip(left_ref, r_to), block).astype(jnp.bfloat16)
            part_copy(c, off).start()

        over_r(other)
        out_ref[:, pl.ds(c * CHUNK, CHUNK)] = product(strip(left_ref, r), block)

    def compute(c):
        if c not in shared:
            main(c, cot_t, hid[c].reshape(G * n, CHUNK))
            return
        b = shared.index(c)

        @pl.when(at_edge)
        def _():
            main(c, cot_own, hid[c, g])

        @pl.when(jnp.logical_not(at_edge))
        def _():
            @pl.when(helper)
            def _():
                block = hid[c, pl.ds(base, G - 1)].reshape((G - 1) * n, CHUNK)
                give_e[b] = product(strip(cot_e, (r + 1) % R), block).astype(jnp.bfloat16)
                swap_e(b).start()
                mine_e[b] = product(strip(cot_e, r), block)

            main(c, cot_t, hid[c].reshape(G * n, CHUNK))

    def hand_over(c):
        b = shared.index(c)

        @pl.when(helper)
        def _():
            swap_e(b).wait_recv()
            sum_e[b] = (mine_e[b] + take_e[b].astype(jnp.float32)).astype(jnp.bfloat16)
            final_e(b, edge).start()

    def tokens_g():
        total = tok_mine[...]
        for off in range(1, G):
            tok_in(off).wait_recv()
            total = total + tok_g[(g + off) % G]
        tok_sum[...] = total
        over_r(lambda off: sum_copy(off).start())

    def add_tokens(off, total):
        sum_in(off).wait_recv()
        return total + tok_r[(r + off) % R]

    inverse = []

    def finish(c):
        cols = pl.ds(c * CHUNK, CHUNK)
        if not inverse:
            total = lax.fori_loop(1, R, add_tokens, tok_sum[...])
            inverse.append((1.0 / total)[0:1, 0:1])

        def add_part(off):
            part_in(c, off).wait_recv()
            out_ref[:, cols] = out_ref[:, cols] + arrived[c, (r + off) % R].astype(jnp.float32)

        over_r(add_part)
        if c in shared:
            b = shared.index(c)

            @pl.when(at_edge)
            def _():
                final_e(b, down).wait_recv()
                out_ref[:, cols] = out_ref[:, cols] + from_e[b].astype(jnp.float32)

        out_ref[:, cols] = out_ref[:, cols] * inverse[0]

    stage = STAGES
    done = []
    ready = 0
    handed = 0
    for t in range(chunks + 1):
        if t < chunks:
            receive(t, 1)
        if t + AHEAD < chunks:
            make_hidden(t + AHEAD)
            send_hidden(t + AHEAD)
        if t == stage[0]:
            share_more()
            tokens_g()
        if t == stage[1]:
            relay_all()
        if t >= 1:
            for k in range(2, G):
                receive(t - 1, k)
        if t == stage[2]:
            turn()
        late = ready
        while t >= stage[2] and ready < t:
            compute(ready)
            ready += 1
        for c in range(handed, late):
            if c in shared:
                hand_over(c)
            handed = c + 1
        if t >= stage[2] + LAG:
            for c in range(t - 1 - LAG):
                if c not in done and c not in shared:
                    finish(c)
                    done.append(c)
    for c in range(handed, chunks):
        if c in shared:
            hand_over(c)
    for c in range(chunks):
        if c not in done:
            finish(c)

    for off in range(1, M):
        spread_copy(off).wait_send()
    for off in range(1, G):
        tok_copy(off).wait_send()
    others(lambda i: direct(i, lambda copy: copy.wait_send()))
    for i in range(G):
        share_drain(cot_all, i, send_3, recv_3)
    if shared:

        @pl.when(g < G - 2)
        def _():
            extra_copy(G - 2, G - 1, 0).wait_send()

        @pl.when(g > 1)
        def _():
            extra_copy(1, 0, 1).wait_send()

        @pl.when(helper)
        def _():
            for i in range(G - 1):
                share_drain(cot_x, base + i, send_y, recv_y)
            for k in range(1, G - 1):
                extra_relay(jnp.where(is_dn, g + k, g - k)).wait_send()
            for b in range(len(shared)):
                swap_e(b).wait_send()
                final_e(b, edge).wait_send()

    for c in range(chunks):
        for i in range(G):

            @pl.when(jnp.logical_and(i <= g, goes_up(c)))
            def _():
                hop(c, i, up, send_up).wait_send()

            @pl.when(jnp.logical_and(i >= g, goes_down(c)))
            def _():
                hop(c, i, down, send_dn).wait_send()

    def drain(off):
        sum_copy(off).wait_send()
        for c in range(chunks):
            part_copy(c, off).wait_send()

    over_r(drain)


def on_device(
    mesh_shape,
    gating_logits,
    lifted_hidden_values,
    loss_output_grad,
    arrival_flags,
    block_owner_map,
    decoder_multipliers,
    block_piece_number,
):
    dp, M = mesh_shape
    G = M
    R = dp // G
    _, slots, toks, width = gating_logits.shape
    feats = loss_output_grad.shape[3]
    rows = feats * M // dp
    chunks = width // CHUNK
    n = slots * toks
    shared = SHARED if R == 2 and G >= 4 else ()
    sizes = (G, R, M, slots, toks, chunks, rows, shared)
    nb = max(len(shared), 1)
    far = G if shared else 1
    smem = pl.BlockSpec(memory_space=pltpu.SMEM)
    vmem = pl.BlockSpec(memory_space=pltpu.VMEM)
    dma = pltpu.SemaphoreType.DMA
    bf, f32 = jnp.bfloat16, jnp.float32
    return pl.pallas_call(
        functools.partial(kernel, sizes),
        out_shape=jax.ShapeDtypeStruct((rows, width), f32),
        in_specs=[smem] * 4 + [pl.BlockSpec(memory_space=pl.ANY)] * 3,
        out_specs=vmem,
        scratch_shapes=[
            pltpu.VMEM((chunks, n, CHUNK), bf),
            pltpu.VMEM((chunks, n, CHUNK), bf),
            pltpu.VMEM((n, feats), bf),
            pltpu.VMEM((M, n // M, feats), bf),
            pltpu.VMEM((chunks, G, n, CHUNK), bf),
            pltpu.VMEM((M, G, n // M, feats), bf),
            pltpu.VMEM((feats, G * n), bf),
            pltpu.VMEM((chunks, R, rows, CHUNK), bf),
            pltpu.VMEM((chunks, R, rows, CHUNK), bf),
            pltpu.VMEM((8, 128), f32),
            pltpu.VMEM((G, 8, 128), f32),
            pltpu.VMEM((8, 128), f32),
            pltpu.VMEM((R, 8, 128), f32),
            pltpu.VMEM((M, far, n // M, feats), bf),
            pltpu.VMEM((feats, n), bf),
            pltpu.VMEM((feats, (G - 1) * n), bf),
            pltpu.VMEM((nb, rows, CHUNK), f32),
            pltpu.VMEM((nb, rows, CHUNK), bf),
            pltpu.VMEM((nb, rows, CHUNK), bf),
            pltpu.VMEM((nb, rows, CHUNK), bf),
            pltpu.VMEM((nb, rows, CHUNK), bf),
            dma,
            dma((chunks,)),
            dma((chunks,)),
            dma((M,)),
            dma((M,)),
            dma((G,)),
            dma((G,)),
            dma((M, G)),
            dma((M, G)),
            dma((chunks, G)),
            dma((chunks, G)),
            dma((chunks, G)),
            dma((chunks, R)),
            dma((chunks, R)),
            dma((G,)),
            dma((G,)),
            dma((R,)),
            dma((R,)),
            dma((2,)),
            dma((G,)),
            dma((M, G)),
            dma((M, G)),
            dma((nb,)),
            dma((nb,)),
            dma((nb,)),
            dma((nb,)),
            dma((G,)),
        ],
        compiler_params=pltpu.CompilerParams(
            collective_id=0, has_side_effects=True
        ),
    )(
        arrival_flags,
        block_owner_map,
        decoder_multipliers,
        block_piece_number,
        gating_logits.reshape(n, width),
        lifted_hidden_values.reshape(n, width),
        loss_output_grad.reshape(n, feats),
    )


def solution(mesh):
    shape = (mesh.shape["dp"], mesh.shape["mp"])
    return jax.shard_map(
        functools.partial(on_device, shape),
        mesh=mesh,
        in_specs=(
            P("dp", None, None, "mp"),
            P("dp", None, None, "mp"),
            P("dp", None, None, "mp"),
            P("dp"),
            P("dp", None),
            P("dp", None),
            P(),
        ),
        out_specs=P("dp", "mp"),
        check_vma=False,
    )
```

```python
import functools

import jax
import jax.numpy as jnp
from jax import lax
from jax.experimental import pallas as pl
from jax.experimental.pallas import tpu as pltpu
from jax.sharding import PartitionSpec as P

TILE = 32
CHUNK = 256
SHARED = (2, 5)
AHEAD = (2, 3, 4)
EARLY = 2
MID = 2
NEXT = 3
STAGES = (0, 0, 2, 2, 3, 5)
EXTRA = (2, 7, 7)
LAG = 1
HAND = 2
TOKENS = 5


def kernel(
    sizes,
    flags_ref,
    owner_ref,
    mult_ref,
    pieces_ref,
    gate_hbm,
    lift_hbm,
    cot_hbm,
    out_ref,
    gate_in,
    lift_in,
    cot_ref,
    quarters,
    hid,
    cot_all,
    cot_t,
    part,
    arrived,
    tok_mine,
    tok_g,
    tok_sum,
    tok_r,
    cot_x,
    cot_own,
    cot_e,
    mine_e,
    give_e,
    take_e,
    sum_e,
    from_e,
    load_c,
    load_g,
    load_l,
    send_1,
    recv_1,
    send_2,
    recv_2,
    send_3,
    recv_3,
    send_up,
    send_dn,
    recv_h,
    send_p,
    recv_p,
    send_tg,
    recv_tg,
    send_tr,
    recv_tr,
    send_x,
    recv_x,
    send_y,
    recv_y,
    send_e,
    recv_e,
    send_f,
    recv_f,
    send_r,
):
    G, R, M, slots, toks, chunks, rows, shared = sizes
    n = slots * toks
    d = lax.axis_index("dp")
    m = lax.axis_index("mp")
    g = d // R
    r = d % R
    quarter = n // M
    pair = M == 4
    m1 = m + 1 - 2 * (m % 2)
    m2 = m + 2 - 4 * (m // 2)
    m3 = m1 + 2 - 4 * (m1 // 2)

    at_edge = jnp.logical_or(g == 0, g == G - 1)
    is_dn = g == 1
    helper = jnp.logical_or(g == 1, g == G - 2)
    base = jnp.where(is_dn, 1, 0)
    edge = jnp.where(is_dn, 0, G - 1)

    def dev(g_to, r_to, m_to):
        return {"dp": g_to * R + r_to, "mp": m_to}

    def remote(src, dst, s, q, where):
        return pltpu.make_async_remote_copy(
            src_ref=src,
            dst_ref=dst,
            send_sem=s,
            recv_sem=q,
            device_id=where,
            device_id_type=pl.DeviceIdType.MESH,
        )

    def spread_copy(off):
        m_to = (m + off) % M
        return remote(
            cot_ref.at[pl.ds(pl.multiple_of(m_to * quarter, quarter), quarter)],
            quarters.at[m],
            send_1.at[off],
            recv_1.at[m],
            dev(g, r, m_to),
        )

    def spread_in(off):
        m_from = (m + off) % M
        return remote(
            quarters.at[m_from],
            quarters.at[m_from],
            send_1.at[off],
            recv_1.at[m_from],
            dev(g, r, m_from),
        )

    def cross_copy(g_to):
        return remote(
            quarters.at[g_to], cot_all.at[m, g], send_2.at[g_to], recv_2.at[g], dev(g_to, r, m)
        )

    def cross_in(g_from):
        return remote(
            quarters.at[g],
            cot_all.at[m, g_from],
            send_2.at[g_from],
            recv_2.at[g_from],
            dev(g_from, r, m),
        )

    def extra_copy(g_to, block, s):
        return remote(
            quarters.at[block], cot_x.at[m, g], send_x.at[s], recv_x.at[g], dev(g_to, r, m)
        )

    def extra_relay(g_from):
        return remote(
            cot_x.at[m, g_from],
            cot_all.at[m, g_from],
            send_r.at[g_from],
            recv_2.at[g_from],
            dev(edge, r, m),
        )

    def extra_in(g_from):
        return remote(
            quarters.at[0], cot_x.at[m, g_from], send_x.at[0], recv_x.at[g_from], dev(g_from, r, m)
        )

    def share(src, buf, origin, i, way, to, sends, recvs):
        return remote(
            src, buf.at[origin, i], sends.at[way, i], recvs.at[origin, i], dev(g, r, to)
        )

    peers = [m1, m2] if pair else [(m + off) % M for off in range(1, M)]

    def share_out(buf, src, i, sends, recvs):
        for way, to in enumerate(peers):
            share(src, buf, m, i, way, to, sends, recvs).start()

    def relay(buf, i, sends, recvs):
        if pair:
            share(buf.at[m2, i], buf, m2, i, 2, m1, sends, recvs).wait_recv()
            share(buf.at[m2, i], buf, m2, i, 2, m1, sends, recvs).start()

    def share_end(buf, i, sends, recvs):
        for o in [m1, m3] if pair else peers:
            share(buf.at[o, i], buf, o, i, 0, m1, sends, recvs).wait_recv()

    def share_drain(buf, i, sends, recvs):
        for way, to in enumerate(peers):
            share(buf.at[m, i], buf, m, i, way, to, sends, recvs).wait_send()
        if pair:
            share(buf.at[m2, i], buf, m2, i, 2, m1, sends, recvs).wait_send()

    def others(reach, body):
        for k in reach:
            if k == 0:
                body(g)
                continue

            @pl.when(g >= k)
            def _():
                body(g - k)

            @pl.when(g + k < G)
            def _():
                body(g + k)

    def extras(body):
        @pl.when(helper)
        def _():
            for k in range(1, G - 1):
                body(jnp.where(is_dn, g + k, g - k))

    def load(src, dst, c, sem):
        return pltpu.make_async_copy(
            src.at[:, pl.ds(c * CHUNK, CHUNK)], dst.at[c], sem.at[c]
        )

    def hop(c, origin, to, sems):
        return remote(
            hid.at[c, origin],
            hid.at[c, origin],
            sems.at[c, origin],
            recv_h.at[c, origin],
            dev(to, r, m),
        )

    up, down = (g + 1) % G, (g + G - 1) % G

    def goes_up(c):
        return g < (G - 2 if c in shared else G - 1)

    def goes_down(c):
        return g > (1 if c in shared else 0)

    def pass_on(c, origin, has_next, to, sems):
        hop(c, origin, to, sems).wait_recv()

        @pl.when(has_next)
        def _():
            hop(c, origin, to, sems).start()

    def receive(c, k):
        from_left = g >= k
        from_right = g + k < G
        if c in shared:
            from_left = jnp.logical_and(from_left, g < G - 1)
            from_right = jnp.logical_and(from_right, g > 0)

        @pl.when(from_left)
        def _():
            pass_on(c, (g + G - k) % G, goes_up(c), up, send_up)

        @pl.when(from_right)
        def _():
            pass_on(c, (g + k) % G, goes_down(c), down, send_dn)

    def part_copy(c, off):
        r_to = (r + off) % R
        return remote(
            part.at[c, r_to], arrived.at[c, r], send_p.at[c, off], recv_p.at[c, r], dev(g, r_to, m)
        )

    def part_in(c, off):
        r_from = (r + off) % R
        return remote(
            part.at[c, r_from],
            arrived.at[c, r_from],
            send_p.at[c, off],
            recv_p.at[c, r_from],
            dev(g, r_from, m),
        )

    def swap_e(b):
        return remote(
            give_e.at[b], take_e.at[b], send_e.at[b], recv_e.at[b], dev(g, (r + 1) % R, m)
        )

    def final_e(b, to):
        return remote(sum_e.at[b], from_e.at[b], send_f.at[b], recv_f.at[b], dev(to, r, m))

    def tok_copy(off):
        return remote(
            tok_mine, tok_g.at[g], send_tg.at[off], recv_tg.at[g], dev((g + off) % G, r, m)
        )

    def tok_in(off):
        g_from = (g + off) % G
        return remote(
            tok_mine, tok_g.at[g_from], send_tg.at[off], recv_tg.at[g_from], dev(g_from, r, m)
        )

    def sum_copy(off):
        return remote(
            tok_sum, tok_r.at[r], send_tr.at[off], recv_tr.at[r], dev(g, (r + off) % R, m)
        )

    def sum_in(off):
        r_from = (r + off) % R
        return remote(
            tok_sum, tok_r.at[r_from], send_tr.at[off], recv_tr.at[r_from], dev(g, r_from, m)
        )

    def over_r(body):
        def step(off, carry):
            body(off)
            return carry

        lax.fori_loop(1, R, step, 0)

    load_cot = pltpu.make_async_copy(cot_hbm, cot_ref, load_c)
    load_cot.start()
    for c in range(chunks):
        load(gate_hbm, gate_in, c, load_g).start()
        load(lift_hbm, lift_in, c, load_l).start()

    barrier = pltpu.get_barrier_semaphore()

    def greet(where):
        pl.semaphore_signal(
            barrier, inc=1, device_id=where, device_id_type=pl.DeviceIdType.MESH
        )

    for off in range(1, M):
        greet(dev(g, r, (m + off) % M))
    for off in range(1, G):
        greet(dev((g + off) % G, r, m))
    over_r(lambda off: greet(dev(g, (r + off) % R, m)))

    flag = flags_ref[0].astype(jnp.float32)
    scales = []
    token_sum = jnp.float32(0)
    row = lax.broadcasted_iota(jnp.int32, (toks, CHUNK), 0)
    for k in range(slots):
        live = pieces_ref[owner_ref[0, k]] * TILE
        weight = flag * mult_ref[0, k].astype(jnp.float32)
        scales.append(jnp.where(row < live, weight, 0.0))
        token_sum = token_sum + weight * live.astype(jnp.float32)
    tok_mine[...] = jnp.full(tok_mine.shape, token_sum, jnp.float32)

    def make_hidden(c):
        load(gate_hbm, gate_in, c, load_g).wait()
        load(lift_hbm, lift_in, c, load_l).wait()
        for k in range(slots):
            rk = pl.ds(k * toks, toks)
            v = gate_in[c, rk, :].astype(jnp.float32)
            u = lift_in[c, rk, :].astype(jnp.float32)
            h = v / (1.0 + jnp.exp(-v)) * u * scales[k]
            hid[c, g, rk, :] = h.astype(jnp.bfloat16)

    if G >= 3:
        up_ways = (
            jnp.logical_and(g >= 1, g < G - 2),
            g == G - 2,
            g == 0,
        )
        down_ways = (
            jnp.logical_and(g > 1, g <= G - 2),
            g == 1,
            g == G - 1,
        )
    else:
        up_ways, down_ways = (g < G - 1,), (g > 0,)
    ways = len(up_ways)
    made = [0]
    sent = [0] * ways

    def send_to(*counts):
        counts = [min(c, chunks) for c in counts[-ways:]]
        for c in range(max(counts)):
            while made[0] <= c:
                make_hidden(made[0])
                made[0] += 1
            for way in range(ways):
                if sent[way] <= c < counts[way] and not (way == 1 and c in shared):

                    @pl.when(up_ways[way])
                    def _():
                        hop(c, g, up, send_up).start()

                    @pl.when(down_ways[way])
                    def _():
                        hop(c, g, down, send_dn).start()

        for way in range(ways):
            sent[way] = max(sent[way], counts[way])

    load_cot.wait()
    quarters[m] = cot_ref[pl.ds(pl.multiple_of(m * quarter, quarter), quarter), :]
    make_hidden(0)
    made[0] = 1
    pl.semaphore_wait(barrier, M - 1 + G - 1 + R - 1)

    for off in range(1, M):
        spread_copy(off).start()
    for off in range(1, G):
        tok_copy(off).start()
    send_to(EARLY, EARLY, EARLY)
    for off in range(1, M):
        spread_in(off).wait_recv()

    def direct(i, body):
        if not shared:
            body(cross_copy(i))
            return
        by_hand = jnp.logical_or(
            jnp.logical_and(i == G - 1, g < G - 2), jnp.logical_and(i == 0, g > 1)
        )

        @pl.when(jnp.logical_not(by_hand))
        def _():
            body(cross_copy(i))

    others(range(G - 1, 0, -1), lambda i: direct(i, lambda copy: copy.start()))
    share_out(cot_all, quarters.at[g], g, send_3, recv_3)
    cot_all[m, g] = quarters[g]
    send_to(MID, MID, MID)
    if shared:

        @pl.when(g < G - 2)
        def _():
            extra_copy(G - 2, G - 1, 0).start()

        @pl.when(g > 1)
        def _():
            extra_copy(1, 0, 1).start()

    send_to(NEXT, NEXT, NEXT)

    def share_cot(reach):
        def one(i):
            cross_in(i).wait_recv()
            share_out(cot_all, cot_all.at[m, i], i, send_3, recv_3)

        others(reach, one)

    def relay_cot(reach):
        others(reach, lambda i: relay(cot_all, i, send_3, recv_3))

    def turn_cot():
        for i in range(G):
            share_end(cot_all, i, send_3, recv_3)
            block = jnp.concatenate([cot_all[j, i] for j in range(M)], axis=0)
            cot_t[:, pl.ds(i * n, n)] = block.T
        if shared:

            @pl.when(at_edge)
            def _():
                block = jnp.concatenate([cot_all[j, g] for j in range(M)], axis=0)
                cot_own[...] = block.T

    def share_extra():
        @pl.when(helper)
        def _():
            share_out(cot_x, quarters.at[edge], g, send_y, recv_y)
            cot_x[m, g] = quarters[edge]

        def more(i):
            extra_in(i).wait_recv()
            extra_relay(i).start()
            share_out(cot_x, cot_x.at[m, i], i, send_y, recv_y)

        extras(more)

    def relay_extra():
        @pl.when(helper)
        def _():
            relay(cot_x, g, send_y, recv_y)

        extras(lambda i: relay(cot_x, i, send_y, recv_y))

    def turn_extra():
        @pl.when(helper)
        def _():
            for i in range(G - 1):
                share_end(cot_x, base + i, send_y, recv_y)
                block = jnp.concatenate([cot_x[j, base + i] for j in range(M)], axis=0)
                cot_e[:, pl.ds(i * n, n)] = block.T

    def product(left, block):
        return jnp.dot(left, block, preferred_element_type=jnp.float32)

    def strip(ref, which):
        return ref[pl.ds(pl.multiple_of(which * rows, rows), rows), :]

    def main(c, left_ref, block):
        def other(off):
            r_to = (r + off) % R
            part[c, r_to] = product(strip(left_ref, r_to), block).astype(jnp.bfloat16)
            part_copy(c, off).start()

        over_r(other)
        out_ref[:, pl.ds(c * CHUNK, CHUNK)] = product(strip(left_ref, r), block)

    def compute(c):
        if c not in shared:
            main(c, cot_t, hid[c].reshape(G * n, CHUNK))
            return
        b = shared.index(c)

        @pl.when(at_edge)
        def _():
            main(c, cot_own, hid[c, g])

        @pl.when(jnp.logical_not(at_edge))
        def _():
            @pl.when(helper)
            def _():
                block = hid[c, pl.ds(base, G - 1)].reshape((G - 1) * n, CHUNK)
                give_e[b] = product(strip(cot_e, (r + 1) % R), block).astype(jnp.bfloat16)
                swap_e(b).start()
                mine_e[b] = product(strip(cot_e, r), block)

            main(c, cot_t, hid[c].reshape(G * n, CHUNK))

    def hand_over(c):
        b = shared.index(c)

        @pl.when(helper)
        def _():
            swap_e(b).wait_recv()
            sum_e[b] = (mine_e[b] + take_e[b].astype(jnp.float32)).astype(jnp.bfloat16)
            final_e(b, edge).start()

    def tokens_g():
        total = tok_mine[...]
        for off in range(1, G):
            tok_in(off).wait_recv()
            total = total + tok_g[(g + off) % G]
        tok_sum[...] = total
        over_r(lambda off: sum_copy(off).start())

    def add_tokens(off, total):
        sum_in(off).wait_recv()
        return total + tok_r[(r + off) % R]

    inverse = []

    def finish(c):
        cols = pl.ds(c * CHUNK, CHUNK)
        if not inverse:
            total = lax.fori_loop(1, R, add_tokens, tok_sum[...])
            inverse.append((1.0 / total)[0:1, 0:1])

        def add_part(off):
            part_in(c, off).wait_recv()
            out_ref[:, cols] = out_ref[:, cols] + arrived[c, (r + off) % R].astype(jnp.float32)

        over_r(add_part)
        if c in shared:
            b = shared.index(c)

            @pl.when(at_edge)
            def _():
                final_e(b, down).wait_recv()
                out_ref[:, cols] = out_ref[:, cols] + from_e[b].astype(jnp.float32)

        out_ref[:, cols] = out_ref[:, cols] * inverse[0]

    near, away = range(1, 2), range(2, G)
    steps = [
        (STAGES[0], lambda: relay_cot(range(1))),
        (STAGES[1], lambda: share_cot(near)),
        (STAGES[2], lambda: share_cot(away)),
        (STAGES[3], lambda: relay_cot(near)),
        (STAGES[4], lambda: relay_cot(away)),
        (STAGES[5], turn_cot),
    ]
    if shared:
        steps.insert(3, (EXTRA[0], share_extra))
        steps.insert(6, (EXTRA[1], relay_extra))
        steps.append((EXTRA[2], turn_extra))
    done = []
    ready = 0
    handed = 0
    start = {}
    for t in range(chunks + 1):
        if t < chunks:
            receive(t, 1)
        send_to(*(t + 1 + ahead for ahead in AHEAD))
        for half in range(2):
            if half and t >= 1:
                for k in range(2, G):
                    receive(t - 1, k)
            for at, step in steps:
                if at == 2 * t + half:
                    step()
            if 2 * t + half == TOKENS:
                tokens_g()
        turned = 2 * t + 1 >= STAGES[5]
        turned_e = 2 * t + 1 >= EXTRA[2]
        while turned and ready < t and (turned_e or ready not in shared):
            compute(ready)
            start[ready] = t
            ready += 1
        while handed < ready and t >= start[handed] + HAND:
            if handed in shared:
                hand_over(handed)
            handed += 1
        if turned and t >= STAGES[5] // 2 + LAG:
            for c in range(min(t - 1 - LAG, ready)):
                if c not in done and c not in shared:
                    finish(c)
                    done.append(c)
    for c in range(handed, chunks):
        if c in shared:
            hand_over(c)
    for c in range(chunks):
        if c not in done:
            finish(c)

    for off in range(1, M):
        spread_copy(off).wait_send()
    for off in range(1, G):
        tok_copy(off).wait_send()
    others(range(1, G), lambda i: direct(i, lambda copy: copy.wait_send()))
    for i in range(G):
        share_drain(cot_all, i, send_3, recv_3)
    if shared:

        @pl.when(g < G - 2)
        def _():
            extra_copy(G - 2, G - 1, 0).wait_send()

        @pl.when(g > 1)
        def _():
            extra_copy(1, 0, 1).wait_send()

        @pl.when(helper)
        def _():
            for i in range(G - 1):
                share_drain(cot_x, base + i, send_y, recv_y)
            for k in range(1, G - 1):
                extra_relay(jnp.where(is_dn, g + k, g - k)).wait_send()
            for b in range(len(shared)):
                swap_e(b).wait_send()
                final_e(b, edge).wait_send()

    for c in range(chunks):
        for i in range(G):

            @pl.when(jnp.logical_and(i <= g, goes_up(c)))
            def _():
                hop(c, i, up, send_up).wait_send()

            @pl.when(jnp.logical_and(i >= g, goes_down(c)))
            def _():
                hop(c, i, down, send_dn).wait_send()

    def drain(off):
        sum_copy(off).wait_send()
        for c in range(chunks):
            part_copy(c, off).wait_send()

    over_r(drain)


def on_device(
    mesh_shape,
    gating_logits,
    lifted_hidden_values,
    loss_output_grad,
    arrival_flags,
    block_owner_map,
    decoder_multipliers,
    block_piece_number,
):
    dp, M = mesh_shape
    G = M
    R = dp // G
    _, slots, toks, width = gating_logits.shape
    feats = loss_output_grad.shape[3]
    rows = feats * M // dp
    chunks = width // CHUNK
    n = slots * toks
    shared = SHARED if R == 2 and G >= 4 else ()
    sizes = (G, R, M, slots, toks, chunks, rows, shared)
    nb = max(len(shared), 1)
    far = G if shared else 1
    smem = pl.BlockSpec(memory_space=pltpu.SMEM)
    vmem = pl.BlockSpec(memory_space=pltpu.VMEM)
    dma = pltpu.SemaphoreType.DMA
    bf, f32 = jnp.bfloat16, jnp.float32
    return pl.pallas_call(
        functools.partial(kernel, sizes),
        out_shape=pltpu.VMEM((rows, width), f32),
        in_specs=[smem] * 4 + [pl.BlockSpec(memory_space=pl.ANY)] * 3,
        out_specs=vmem,
        scratch_shapes=[
            pltpu.VMEM((chunks, n, CHUNK), bf),
            pltpu.VMEM((chunks, n, CHUNK), bf),
            pltpu.VMEM((n, feats), bf),
            pltpu.VMEM((M, n // M, feats), bf),
            pltpu.VMEM((chunks, G, n, CHUNK), bf),
            pltpu.VMEM((M, G, n // M, feats), bf),
            pltpu.VMEM((feats, G * n), bf),
            pltpu.VMEM((chunks, R, rows, CHUNK), bf),
            pltpu.VMEM((chunks, R, rows, CHUNK), bf),
            pltpu.VMEM((8, 128), f32),
            pltpu.VMEM((G, 8, 128), f32),
            pltpu.VMEM((8, 128), f32),
            pltpu.VMEM((R, 8, 128), f32),
            pltpu.VMEM((M, far, n // M, feats), bf),
            pltpu.VMEM((feats, n), bf),
            pltpu.VMEM((feats, (G - 1) * n), bf),
            pltpu.VMEM((nb, rows, CHUNK), f32),
            pltpu.VMEM((nb, rows, CHUNK), bf),
            pltpu.VMEM((nb, rows, CHUNK), bf),
            pltpu.VMEM((nb, rows, CHUNK), bf),
            pltpu.VMEM((nb, rows, CHUNK), bf),
            dma,
            dma((chunks,)),
            dma((chunks,)),
            dma((M,)),
            dma((M,)),
            dma((G,)),
            dma((G,)),
            dma((M, G)),
            dma((M, G)),
            dma((chunks, G)),
            dma((chunks, G)),
            dma((chunks, G)),
            dma((chunks, R)),
            dma((chunks, R)),
            dma((G,)),
            dma((G,)),
            dma((R,)),
            dma((R,)),
            dma((2,)),
            dma((G,)),
            dma((M, G)),
            dma((M, G)),
            dma((nb,)),
            dma((nb,)),
            dma((nb,)),
            dma((nb,)),
            dma((G,)),
        ],
        compiler_params=pltpu.CompilerParams(
            collective_id=0, has_side_effects=True, vmem_limit_bytes=58_000_000
        ),
    )(
        arrival_flags,
        block_owner_map,
        decoder_multipliers,
        block_piece_number,
        gating_logits.reshape(n, width),
        lifted_hidden_values.reshape(n, width),
        loss_output_grad.reshape(n, feats),
    )


def solution(mesh):
    shape = (mesh.shape["dp"], mesh.shape["mp"])
    return jax.shard_map(
        functools.partial(on_device, shape),
        mesh=mesh,
        in_specs=(
            P("dp", None, None, "mp"),
            P("dp", None, None, "mp"),
            P("dp", None, None, "mp"),
            P("dp"),
            P("dp", None),
            P("dp", None),
            P(),
        ),
        out_specs=P("dp", "mp"),
        check_vma=False,
    )
```

```python
import functools

import jax
import jax.numpy as jnp
from jax import lax
from jax.experimental import pallas as pl
from jax.experimental.pallas import tpu as pltpu
from jax.sharding import PartitionSpec as P

TILE = 32
CHUNK = 256
LANES = 128
HEAD = 1
TAIL = 3
SHARED = (2, 6, 7)
AHEAD = (2, 1, 7)
EARLY = (3, 4, 2)
MID = (2, 7, 1)
NEXT = (3, 7, 5)
STAGES = (4, 0, 0, 2, 4, 4)
EXTRA = (2, 6, 7)
LAG = 5
HAND = 3
TOKENS = 4


def chunk_widths(width):
    full, rest = divmod(width - LANES * (HEAD + TAIL), CHUNK)
    return (LANES,) * HEAD + (CHUNK,) * full + (LANES,) * (TAIL + rest // LANES)


def kernel(
    sizes,
    flags_hbm,
    owner_hbm,
    mult_hbm,
    pieces_hbm,
    gate_hbm,
    lift_hbm,
    cot_hbm,
    out_ref,
    gate_in,
    lift_in,
    cot_ref,
    quarters,
    hid,
    cot_all,
    cot_t,
    part,
    arrived,
    tok_mine,
    tok_g,
    tok_sum,
    tok_r,
    cot_x,
    cot_own,
    cot_e,
    mine_e,
    give_e,
    take_e,
    sum_e,
    from_e,
    load_c,
    load_g,
    load_l,
    send_1,
    recv_1,
    send_2,
    recv_2,
    send_3,
    recv_3,
    send_up,
    send_dn,
    recv_h,
    send_p,
    recv_p,
    send_tg,
    recv_tg,
    send_tr,
    recv_tr,
    send_x,
    recv_x,
    send_y,
    recv_y,
    send_e,
    recv_e,
    send_f,
    recv_f,
    send_r,
    flags_ref,
    owner_ref,
    mult_ref,
    pieces_ref,
    load_s,
):
    G, R, M, slots, toks, widths, rows, shared = sizes
    chunks = len(widths)
    starts = [sum(widths[:c]) for c in range(chunks)]
    wide = max(widths)
    n = slots * toks
    d = lax.axis_index("dp")
    m = lax.axis_index("mp")
    g = d // R
    r = d % R
    quarter = n // M
    pair = M == 4
    m1 = m + 1 - 2 * (m % 2)
    m2 = m + 2 - 4 * (m // 2)
    m3 = m1 + 2 - 4 * (m1 // 2)

    at_edge = jnp.logical_or(g == 0, g == G - 1)
    is_dn = g == 1
    helper = jnp.logical_or(g == 1, g == G - 2)
    base = jnp.where(is_dn, 1, 0)
    edge = jnp.where(is_dn, 0, G - 1)

    def dev(g_to, r_to, m_to):
        return {"dp": g_to * R + r_to, "mp": m_to}

    def remote(src, dst, s, q, where):
        return pltpu.make_async_remote_copy(
            src_ref=src,
            dst_ref=dst,
            send_sem=s,
            recv_sem=q,
            device_id=where,
            device_id_type=pl.DeviceIdType.MESH,
        )

    def spread_copy(off):
        m_to = (m + off) % M
        return remote(
            cot_ref.at[pl.ds(pl.multiple_of(m_to * quarter, quarter), quarter)],
            quarters.at[m],
            send_1.at[off],
            recv_1.at[m],
            dev(g, r, m_to),
        )

    def spread_in(off):
        m_from = (m + off) % M
        return remote(
            quarters.at[m_from],
            quarters.at[m_from],
            send_1.at[off],
            recv_1.at[m_from],
            dev(g, r, m_from),
        )

    def cross_copy(g_to):
        return remote(
            quarters.at[g_to], cot_all.at[m, g], send_2.at[g_to], recv_2.at[g], dev(g_to, r, m)
        )

    def cross_in(g_from):
        return remote(
            quarters.at[g],
            cot_all.at[m, g_from],
            send_2.at[g_from],
            recv_2.at[g_from],
            dev(g_from, r, m),
        )

    def extra_copy(g_to, block, s):
        return remote(
            quarters.at[block], cot_x.at[m, g], send_x.at[s], recv_x.at[g], dev(g_to, r, m)
        )

    def extra_relay(g_from):
        return remote(
            cot_x.at[m, g_from],
            cot_all.at[m, g_from],
            send_r.at[g_from],
            recv_2.at[g_from],
            dev(edge, r, m),
        )

    def extra_in(g_from):
        return remote(
            quarters.at[0], cot_x.at[m, g_from], send_x.at[0], recv_x.at[g_from], dev(g_from, r, m)
        )

    def share(src, buf, origin, i, way, to, sends, recvs):
        return remote(
            src, buf.at[origin, i], sends.at[way, i], recvs.at[origin, i], dev(g, r, to)
        )

    peers = [m1, m2] if pair else [(m + off) % M for off in range(1, M)]

    def share_out(buf, src, i, sends, recvs):
        for way, to in enumerate(peers):
            share(src, buf, m, i, way, to, sends, recvs).start()

    def relay(buf, i, sends, recvs):
        if pair:
            share(buf.at[m2, i], buf, m2, i, 2, m1, sends, recvs).wait_recv()
            share(buf.at[m2, i], buf, m2, i, 2, m1, sends, recvs).start()

    def share_end(buf, i, sends, recvs):
        for o in [m1, m3] if pair else peers:
            share(buf.at[o, i], buf, o, i, 0, m1, sends, recvs).wait_recv()

    def share_drain(buf, i, sends, recvs):
        for way, to in enumerate(peers):
            share(buf.at[m, i], buf, m, i, way, to, sends, recvs).wait_send()
        if pair:
            share(buf.at[m2, i], buf, m2, i, 2, m1, sends, recvs).wait_send()

    def others(reach, body):
        for k in reach:
            if k == 0:
                body(g)
                continue

            @pl.when(g >= k)
            def _():
                body(g - k)

            @pl.when(g + k < G)
            def _():
                body(g + k)

    def extras(body):
        @pl.when(helper)
        def _():
            for k in range(1, G - 1):
                body(jnp.where(is_dn, g + k, g - k))

    def cut(ref, c, *index):
        if widths[c] == wide:
            return ref.at[index]
        return ref.at[(*index, slice(None), pl.ds(0, widths[c]))]

    def columns(c):
        return pl.ds(starts[c], widths[c])

    def load(src, dst, c, sem):
        return pltpu.make_async_copy(
            src.at[:, columns(c)], cut(dst, c, c), sem.at[c]
        )

    def hop(c, origin, to, sems):
        return remote(
            cut(hid, c, c, origin),
            cut(hid, c, c, origin),
            sems.at[c, origin],
            recv_h.at[c, origin],
            dev(to, r, m),
        )

    up, down = (g + 1) % G, (g + G - 1) % G

    def goes_up(c):
        return g < (G - 2 if c in shared else G - 1)

    def goes_down(c):
        return g > (1 if c in shared else 0)

    def pass_on(c, origin, has_next, to, sems):
        hop(c, origin, to, sems).wait_recv()

        @pl.when(has_next)
        def _():
            hop(c, origin, to, sems).start()

    def receive(c, k):
        from_left = g >= k
        from_right = g + k < G
        if c in shared:
            from_left = jnp.logical_and(from_left, g < G - 1)
            from_right = jnp.logical_and(from_right, g > 0)

        @pl.when(from_left)
        def _():
            pass_on(c, (g + G - k) % G, goes_up(c), up, send_up)

        @pl.when(from_right)
        def _():
            pass_on(c, (g + k) % G, goes_down(c), down, send_dn)

    def part_copy(c, off):
        r_to = (r + off) % R
        return remote(
            cut(part, c, c, r_to),
            cut(arrived, c, c, r),
            send_p.at[c, off],
            recv_p.at[c, r],
            dev(g, r_to, m),
        )

    def part_in(c, off):
        r_from = (r + off) % R
        return remote(
            cut(part, c, c, r_from),
            cut(arrived, c, c, r_from),
            send_p.at[c, off],
            recv_p.at[c, r_from],
            dev(g, r_from, m),
        )

    def swap_e(b):
        return remote(
            cut(give_e, shared[b], b),
            cut(take_e, shared[b], b),
            send_e.at[b],
            recv_e.at[b],
            dev(g, (r + 1) % R, m),
        )

    def final_e(b, to):
        return remote(
            cut(sum_e, shared[b], b),
            cut(from_e, shared[b], b),
            send_f.at[b],
            recv_f.at[b],
            dev(to, r, m),
        )

    def tok_copy(off):
        return remote(
            tok_mine, tok_g.at[g], send_tg.at[off], recv_tg.at[g], dev((g + off) % G, r, m)
        )

    def tok_in(off):
        g_from = (g + off) % G
        return remote(
            tok_mine, tok_g.at[g_from], send_tg.at[off], recv_tg.at[g_from], dev(g_from, r, m)
        )

    def sum_copy(off):
        return remote(
            tok_sum, tok_r.at[r], send_tr.at[off], recv_tr.at[r], dev(g, (r + off) % R, m)
        )

    def sum_in(off):
        r_from = (r + off) % R
        return remote(
            tok_sum, tok_r.at[r_from], send_tr.at[off], recv_tr.at[r_from], dev(g, r_from, m)
        )

    def over_r(body):
        def step(off, carry):
            body(off)
            return carry

        lax.fori_loop(1, R, step, 0)

    small = [
        pltpu.make_async_copy(a, b, load_s.at[i])
        for i, (a, b) in enumerate(
            (
                (flags_hbm, flags_ref),
                (owner_hbm, owner_ref),
                (mult_hbm, mult_ref),
                (pieces_hbm, pieces_ref),
            )
        )
    ]
    for copy in small:
        copy.start()
    load_cot = pltpu.make_async_copy(cot_hbm, cot_ref, load_c)
    load_cot.start()
    for c in range(chunks):
        load(gate_hbm, gate_in, c, load_g).start()
        load(lift_hbm, lift_in, c, load_l).start()

    barrier = pltpu.get_barrier_semaphore()

    def greet(where):
        pl.semaphore_signal(
            barrier, inc=1, device_id=where, device_id_type=pl.DeviceIdType.MESH
        )

    for off in range(1, M):
        greet(dev(g, r, (m + off) % M))
    for off in range(1, G):
        greet(dev((g + off) % G, r, m))
    over_r(lambda off: greet(dev(g, (r + off) % R, m)))

    for copy in small:
        copy.wait()
    flag = flags_ref[0].astype(jnp.float32)
    scales = []
    token_sum = jnp.float32(0)
    row = lax.broadcasted_iota(jnp.int32, (toks, wide), 0)
    for k in range(slots):
        live = pieces_ref[owner_ref[0, k]] * TILE
        weight = flag * mult_ref[0, k].astype(jnp.float32)
        scales.append(jnp.where(row < live, weight, 0.0))
        token_sum = token_sum + weight * live.astype(jnp.float32)
    tok_mine[...] = jnp.full(tok_mine.shape, token_sum, jnp.float32)

    def make_hidden(c):
        load(gate_hbm, gate_in, c, load_g).wait()
        load(lift_hbm, lift_in, c, load_l).wait()
        for k in range(slots):
            rk = pl.ds(k * toks, toks)
            cols = pl.ds(0, widths[c])
            v = gate_in[c, rk, cols].astype(jnp.float32)
            u = lift_in[c, rk, cols].astype(jnp.float32)
            h = v / (1.0 + jnp.exp(-v)) * u * scales[k][:, : widths[c]]
            hid[c, g, rk, cols] = h.astype(jnp.bfloat16)

    if G >= 3:
        up_ways = (
            jnp.logical_and(g >= 1, g < G - 2),
            g == G - 2,
            g == 0,
        )
        down_ways = (
            jnp.logical_and(g > 1, g <= G - 2),
            g == 1,
            g == G - 1,
        )
    else:
        up_ways, down_ways = (g < G - 1,), (g > 0,)
    ways = len(up_ways)
    made = [0]
    sent = [0] * ways

    def send_to(*counts):
        counts = [min(c, chunks) for c in counts[-ways:]]
        for c in range(max(counts)):
            while made[0] <= c:
                make_hidden(made[0])
                made[0] += 1
            for way in range(ways):
                if sent[way] <= c < counts[way] and not (way == 1 and c in shared):

                    @pl.when(up_ways[way])
                    def _():
                        hop(c, g, up, send_up).start()

                    @pl.when(down_ways[way])
                    def _():
                        hop(c, g, down, send_dn).start()

        for way in range(ways):
            sent[way] = max(sent[way], counts[way])

    load_cot.wait()
    quarters[m] = cot_ref[pl.ds(pl.multiple_of(m * quarter, quarter), quarter), :]
    make_hidden(0)
    made[0] = 1
    pl.semaphore_wait(barrier, M - 1 + G - 1 + R - 1)

    for off in range(1, M):
        spread_copy(off).start()
    for off in range(1, G):
        tok_copy(off).start()
    send_to(*EARLY)
    for off in range(1, M):
        spread_in(off).wait_recv()

    def direct(i, body):
        if not shared:
            body(cross_copy(i))
            return
        by_hand = jnp.logical_or(
            jnp.logical_and(i == G - 1, g < G - 2), jnp.logical_and(i == 0, g > 1)
        )

        @pl.when(jnp.logical_not(by_hand))
        def _():
            body(cross_copy(i))

    others(range(G - 1, 0, -1), lambda i: direct(i, lambda copy: copy.start()))
    share_out(cot_all, quarters.at[g], g, send_3, recv_3)
    cot_all[m, g] = quarters[g]
    send_to(*MID)

    def share_cot(reach):
        def one(i):
            cross_in(i).wait_recv()
            share_out(cot_all, cot_all.at[m, i], i, send_3, recv_3)

        others(reach, one)

    if STAGES[1] < 0:
        share_cot(range(1, 2))
    if shared:

        @pl.when(g < G - 2)
        def _():
            extra_copy(G - 2, G - 1, 0).start()

        @pl.when(g > 1)
        def _():
            extra_copy(1, 0, 1).start()

    send_to(*NEXT)

    def relay_cot(reach):
        others(reach, lambda i: relay(cot_all, i, send_3, recv_3))

    def turn_cot():
        for i in range(G):
            share_end(cot_all, i, send_3, recv_3)
            block = jnp.concatenate([cot_all[j, i] for j in range(M)], axis=0)
            cot_t[:, pl.ds(i * n, n)] = block.T
        if shared:

            @pl.when(at_edge)
            def _():
                block = jnp.concatenate([cot_all[j, g] for j in range(M)], axis=0)
                cot_own[...] = block.T

    def share_extra():
        @pl.when(helper)
        def _():
            share_out(cot_x, quarters.at[edge], g, send_y, recv_y)
            cot_x[m, g] = quarters[edge]

        def more(i):
            extra_in(i).wait_recv()
            extra_relay(i).start()
            share_out(cot_x, cot_x.at[m, i], i, send_y, recv_y)

        extras(more)

    def relay_extra():
        @pl.when(helper)
        def _():
            relay(cot_x, g, send_y, recv_y)

        extras(lambda i: relay(cot_x, i, send_y, recv_y))

    def turn_extra():
        @pl.when(helper)
        def _():
            for i in range(G - 1):
                share_end(cot_x, base + i, send_y, recv_y)
                block = jnp.concatenate([cot_x[j, base + i] for j in range(M)], axis=0)
                cot_e[:, pl.ds(i * n, n)] = block.T

    def product(left, block):
        return jnp.dot(left, block, preferred_element_type=jnp.float32)

    def strip(ref, which):
        return ref[pl.ds(pl.multiple_of(which * rows, rows), rows), :]

    def main(c, left_ref, block):
        def other(off):
            r_to = (r + off) % R
            cut(part, c, c, r_to)[...] = product(strip(left_ref, r_to), block).astype(
                jnp.bfloat16
            )
            part_copy(c, off).start()

        over_r(other)
        out_ref[:, columns(c)] = product(strip(left_ref, r), block)

    def every(c):
        return hid[c, :, :, pl.ds(0, widths[c])].reshape(G * n, widths[c])

    def compute(c):
        if c not in shared:
            main(c, cot_t, every(c))
            return
        b = shared.index(c)

        @pl.when(at_edge)
        def _():
            main(c, cot_own, hid[c, g, :, pl.ds(0, widths[c])])

        @pl.when(jnp.logical_not(at_edge))
        def _():
            @pl.when(helper)
            def _():
                block = hid[c, pl.ds(base, G - 1), :, pl.ds(0, widths[c])]
                block = block.reshape((G - 1) * n, widths[c])
                cut(give_e, c, b)[...] = product(strip(cot_e, (r + 1) % R), block).astype(
                    jnp.bfloat16
                )
                swap_e(b).start()
                cut(mine_e, c, b)[...] = product(strip(cot_e, r), block)

            main(c, cot_t, every(c))

    def hand_over(c):
        b = shared.index(c)

        @pl.when(helper)
        def _():
            swap_e(b).wait_recv()
            total = cut(mine_e, c, b)[...] + cut(take_e, c, b)[...].astype(jnp.float32)
            cut(sum_e, c, b)[...] = total.astype(jnp.bfloat16)
            final_e(b, edge).start()

    def tokens_g():
        total = tok_mine[...]
        for off in range(1, G):
            tok_in(off).wait_recv()
            total = total + tok_g[(g + off) % G]
        tok_sum[...] = total
        over_r(lambda off: sum_copy(off).start())

    def add_tokens(off, total):
        sum_in(off).wait_recv()
        return total + tok_r[(r + off) % R]

    inverse = []

    def finish(c):
        cols = columns(c)
        if not inverse:
            total = lax.fori_loop(1, R, add_tokens, tok_sum[...])
            inverse.append((1.0 / total)[0:1, 0:1])

        def add_part(off):
            part_in(c, off).wait_recv()
            out_ref[:, cols] = out_ref[:, cols] + cut(arrived, c, c, (r + off) % R)[
                ...
            ].astype(jnp.float32)

        over_r(add_part)
        if c in shared:
            b = shared.index(c)

            @pl.when(at_edge)
            def _():
                final_e(b, down).wait_recv()
                out_ref[:, cols] = out_ref[:, cols] + cut(from_e, c, b)[...].astype(jnp.float32)

        out_ref[:, cols] = out_ref[:, cols] * inverse[0]

    near, away = range(1, 2), range(2, G)
    steps = [
        (STAGES[0], lambda: relay_cot(range(1))),
        (STAGES[1], lambda: share_cot(near)),
        (STAGES[2], lambda: share_cot(away)),
        (STAGES[3], lambda: relay_cot(near)),
        (STAGES[4], lambda: relay_cot(away)),
        (STAGES[5], turn_cot),
    ]
    if shared:
        steps.insert(3, (EXTRA[0], share_extra))
        steps.insert(6, (EXTRA[1], relay_extra))
        steps.append((EXTRA[2], turn_extra))
    done = []
    ready = 0
    handed = 0
    start = {}
    for t in range(chunks + 1):
        if t < chunks:
            receive(t, 1)
        send_to(*(t + 1 + ahead for ahead in AHEAD))
        for half in range(2):
            if half and t >= 1:
                for k in range(2, G):
                    receive(t - 1, k)
            for at, step in steps:
                if at == 2 * t + half:
                    step()
            if 2 * t + half == TOKENS:
                tokens_g()
        turned = 2 * t + 1 >= STAGES[5]
        turned_e = 2 * t + 1 >= EXTRA[2]
        while turned and ready < t and (turned_e or ready not in shared):
            compute(ready)
            start[ready] = t
            ready += 1
        while handed < ready and t >= start[handed] + HAND:
            if handed in shared:
                hand_over(handed)
            handed += 1
        if turned and t >= STAGES[5] // 2 + LAG:
            for c in range(min(t - 1 - LAG, ready)):
                if c not in done and c not in shared:
                    finish(c)
                    done.append(c)
    for c in range(handed, chunks):
        if c in shared:
            hand_over(c)
    for c in range(chunks):
        if c not in done:
            finish(c)

    for off in range(1, M):
        spread_copy(off).wait_send()
    for off in range(1, G):
        tok_copy(off).wait_send()
    others(range(1, G), lambda i: direct(i, lambda copy: copy.wait_send()))
    for i in range(G):
        share_drain(cot_all, i, send_3, recv_3)
    if shared:

        @pl.when(g < G - 2)
        def _():
            extra_copy(G - 2, G - 1, 0).wait_send()

        @pl.when(g > 1)
        def _():
            extra_copy(1, 0, 1).wait_send()

        @pl.when(helper)
        def _():
            for i in range(G - 1):
                share_drain(cot_x, base + i, send_y, recv_y)
            for k in range(1, G - 1):
                extra_relay(jnp.where(is_dn, g + k, g - k)).wait_send()
            for b in range(len(shared)):
                swap_e(b).wait_send()
                final_e(b, edge).wait_send()

    for c in range(chunks):
        for i in range(G):

            @pl.when(jnp.logical_and(i <= g, goes_up(c)))
            def _():
                hop(c, i, up, send_up).wait_send()

            @pl.when(jnp.logical_and(i >= g, goes_down(c)))
            def _():
                hop(c, i, down, send_dn).wait_send()

    def drain(off):
        sum_copy(off).wait_send()
        for c in range(chunks):
            part_copy(c, off).wait_send()

    over_r(drain)


def on_device(
    mesh_shape,
    gating_logits,
    lifted_hidden_values,
    loss_output_grad,
    arrival_flags,
    block_owner_map,
    decoder_multipliers,
    block_piece_number,
):
    dp, M = mesh_shape
    G = M
    R = dp // G
    _, slots, toks, width = gating_logits.shape
    feats = loss_output_grad.shape[3]
    rows = feats * M // dp
    widths = chunk_widths(width)
    chunks = len(widths)
    wide = max(widths)
    n = slots * toks
    shared = SHARED if R == 2 and G >= 4 else ()
    sizes = (G, R, M, slots, toks, widths, rows, shared)
    nb = max(len(shared), 1)
    far = G if shared else 1
    vmem = pl.BlockSpec(memory_space=pltpu.VMEM)
    dma = pltpu.SemaphoreType.DMA
    bf, f32 = jnp.bfloat16, jnp.float32
    return pl.pallas_call(
        functools.partial(kernel, sizes),
        out_shape=pltpu.VMEM((rows, width), f32),
        in_specs=[pl.BlockSpec(memory_space=pl.ANY)] * 7,
        out_specs=vmem,
        scratch_shapes=[
            pltpu.VMEM((chunks, n, wide), bf),
            pltpu.VMEM((chunks, n, wide), bf),
            pltpu.VMEM((n, feats), bf),
            pltpu.VMEM((M, n // M, feats), bf),
            pltpu.VMEM((chunks, G, n, wide), bf),
            pltpu.VMEM((M, G, n // M, feats), bf),
            pltpu.VMEM((feats, G * n), bf),
            pltpu.VMEM((chunks, R, rows, wide), bf),
            pltpu.VMEM((chunks, R, rows, wide), bf),
            pltpu.VMEM((8, 128), f32),
            pltpu.VMEM((G, 8, 128), f32),
            pltpu.VMEM((8, 128), f32),
            pltpu.VMEM((R, 8, 128), f32),
            pltpu.VMEM((M, far, n // M, feats), bf),
            pltpu.VMEM((feats, n), bf),
            pltpu.VMEM((feats, (G - 1) * n), bf),
            pltpu.VMEM((nb, rows, wide), f32),
            pltpu.VMEM((nb, rows, wide), bf),
            pltpu.VMEM((nb, rows, wide), bf),
            pltpu.VMEM((nb, rows, wide), bf),
            pltpu.VMEM((nb, rows, wide), bf),
            dma,
            dma((chunks,)),
            dma((chunks,)),
            dma((M,)),
            dma((M,)),
            dma((G,)),
            dma((G,)),
            dma((M, G)),
            dma((M, G)),
            dma((chunks, G)),
            dma((chunks, G)),
            dma((chunks, G)),
            dma((chunks, R)),
            dma((chunks, R)),
            dma((G,)),
            dma((G,)),
            dma((R,)),
            dma((R,)),
            dma((2,)),
            dma((G,)),
            dma((M, G)),
            dma((M, G)),
            dma((nb,)),
            dma((nb,)),
            dma((nb,)),
            dma((nb,)),
            dma((G,)),
            pltpu.SMEM(arrival_flags.shape, jnp.int32),
            pltpu.SMEM(block_owner_map.shape, jnp.int32),
            pltpu.SMEM(decoder_multipliers.shape, jnp.int32),
            pltpu.SMEM(block_piece_number.shape, jnp.int32),
            dma((4,)),
        ],
        compiler_params=pltpu.CompilerParams(
            collective_id=0, has_side_effects=True, vmem_limit_bytes=58_000_000
        ),
    )(
        arrival_flags,
        block_owner_map,
        decoder_multipliers,
        block_piece_number,
        gating_logits.reshape(n, width),
        lifted_hidden_values.reshape(n, width),
        loss_output_grad.reshape(n, feats),
    )


def solution(mesh):
    shape = (mesh.shape["dp"], mesh.shape["mp"])
    return jax.shard_map(
        functools.partial(on_device, shape),
        mesh=mesh,
        in_specs=(
            P("dp", None, None, "mp"),
            P("dp", None, None, "mp"),
            P("dp", None, None, "mp"),
            P("dp"),
            P("dp", None),
            P("dp", None),
            P(),
        ),
        out_specs=P("dp", "mp"),
        check_vma=False,
    )
```

```python
import functools

import jax
import jax.numpy as jnp
from jax import lax
from jax.experimental import pallas as pl
from jax.experimental.pallas import tpu as pltpu
from jax.sharding import PartitionSpec as P

TILE = 32
CHUNK = 256
LANES = 128
HEAD = 2
TAIL = 4
SHARED = (2, 4, 6, 7, 8)
RETURNED = (3, 5)
AHEAD = (2, 9, 8)
EARLY = (3, 4, 2)
MID = (2, 6, 2)
NEXT = (1, 2, 1)
STAGES = (2, 0, 2, 3, 4, 4)
EXTRA = (2, 7, 7)
LAG = 5
HAND = 2
TOKENS = 4


def chunk_widths(width):
    full, rest = divmod(width - LANES * (HEAD + TAIL), CHUNK)
    return (LANES,) * HEAD + (CHUNK,) * full + (LANES,) * (TAIL + rest // LANES)


def kernel(
    sizes,
    flags_hbm,
    owner_hbm,
    mult_hbm,
    pieces_hbm,
    gate_hbm,
    lift_hbm,
    cot_hbm,
    out_ref,
    gate_in,
    lift_in,
    cot_ref,
    quarters,
    hid,
    cot_all,
    cot_t,
    part,
    arrived,
    tok_mine,
    tok_g,
    tok_sum,
    tok_r,
    cot_x,
    cot_e,
    mine_e,
    give_e,
    take_e,
    sum_e,
    from_e,
    load_c,
    load_g,
    load_l,
    send_1,
    recv_1,
    send_2,
    recv_2,
    send_3,
    recv_3,
    send_up,
    send_dn,
    recv_h,
    send_p,
    recv_p,
    send_tg,
    recv_tg,
    send_tr,
    recv_tr,
    send_x,
    recv_x,
    send_y,
    recv_y,
    send_e,
    recv_e,
    send_f,
    recv_f,
    send_r,
    send_s,
    flags_ref,
    owner_ref,
    mult_ref,
    pieces_ref,
    load_s,
):
    G, R, M, slots, toks, widths, rows, shared, returned = sizes
    chunks = len(widths)
    starts = [sum(widths[:c]) for c in range(chunks)]
    wide = max(widths)
    n = slots * toks
    d = lax.axis_index("dp")
    m = lax.axis_index("mp")
    g = d // R
    r = d % R
    quarter = n // M
    pair = M == 4
    m1 = m + 1 - 2 * (m % 2)
    m2 = m + 2 - 4 * (m // 2)
    m3 = m1 + 2 - 4 * (m1 // 2)

    at_edge = jnp.logical_or(g == 0, g == G - 1)
    helper = jnp.logical_not(at_edge)
    buddy = g + 1 - 2 * (g % 2)
    paired = shared + returned

    def dev(g_to, r_to, m_to):
        return {"dp": g_to * R + r_to, "mp": m_to}

    def remote(src, dst, s, q, where):
        return pltpu.make_async_remote_copy(
            src_ref=src,
            dst_ref=dst,
            send_sem=s,
            recv_sem=q,
            device_id=where,
            device_id_type=pl.DeviceIdType.MESH,
        )

    def spread_copy(off):
        m_to = (m + off) % M
        return remote(
            cot_ref.at[pl.ds(pl.multiple_of(m_to * quarter, quarter), quarter)],
            quarters.at[m],
            send_1.at[off],
            recv_1.at[m],
            dev(g, r, m_to),
        )

    def spread_in(off):
        m_from = (m + off) % M
        return remote(
            quarters.at[m_from],
            quarters.at[m_from],
            send_1.at[off],
            recv_1.at[m_from],
            dev(g, r, m_from),
        )

    def cross_copy(g_to):
        return remote(
            quarters.at[g_to], cot_all.at[m, g], send_2.at[g_to], recv_2.at[g], dev(g_to, r, m)
        )

    def cross_in(g_from):
        return remote(
            quarters.at[g],
            cot_all.at[m, g_from],
            send_2.at[g_from],
            recv_2.at[g_from],
            dev(g_from, r, m),
        )

    def extra_copy(g_to):
        return remote(
            quarters.at[g_to + 1 - 2 * (g_to % 2)],
            cot_x.at[m, g],
            send_x.at[g_to],
            recv_x.at[g],
            dev(g_to, r, m),
        )

    def pass_cot(g_from):
        return remote(
            cot_x.at[m, g_from],
            cot_all.at[m, g_from],
            send_r.at[g_from],
            recv_2.at[g_from],
            dev(buddy, r, m),
        )

    def pass_extra(g_from):
        return remote(
            cot_all.at[m, g_from],
            cot_x.at[m, g_from],
            send_s.at[g_from],
            recv_x.at[g_from],
            dev(buddy, r, m),
        )

    def extra_in(g_from):
        return remote(
            quarters.at[0], cot_x.at[m, g_from], send_x.at[0], recv_x.at[g_from], dev(g_from, r, m)
        )

    def share(src, buf, origin, i, way, to, sends, recvs):
        return remote(
            src, buf.at[origin, i], sends.at[way, i], recvs.at[origin, i], dev(g, r, to)
        )

    peers = [m1, m2] if pair else [(m + off) % M for off in range(1, M)]

    def share_out(buf, src, i, sends, recvs):
        for way, to in enumerate(peers):
            share(src, buf, m, i, way, to, sends, recvs).start()

    def relay(buf, i, sends, recvs):
        if pair:
            share(buf.at[m2, i], buf, m2, i, 2, m1, sends, recvs).wait_recv()
            share(buf.at[m2, i], buf, m2, i, 2, m1, sends, recvs).start()

    def share_end(buf, i, sends, recvs):
        for o in [m1, m3] if pair else peers:
            share(buf.at[o, i], buf, o, i, 0, m1, sends, recvs).wait_recv()

    def share_drain(buf, i, sends, recvs):
        for way, to in enumerate(peers):
            share(buf.at[m, i], buf, m, i, way, to, sends, recvs).wait_send()
        if pair:
            share(buf.at[m2, i], buf, m2, i, 2, m1, sends, recvs).wait_send()

    def others(reach, body):
        for k in reach:
            if k == 0:
                body(g)
                continue

            @pl.when(g >= k)
            def _():
                body(g - k)

            @pl.when(g + k < G)
            def _():
                body(g + k)

    def cut(ref, c, *index):
        if widths[c] == wide:
            return ref.at[index]
        return ref.at[(*index, slice(None), pl.ds(0, widths[c]))]

    def columns(c):
        return pl.ds(starts[c], widths[c])

    def load(src, dst, c, sem):
        return pltpu.make_async_copy(
            src.at[:, columns(c)], cut(dst, c, c), sem.at[c]
        )

    def hop(c, origin, to, sems):
        return remote(
            cut(hid, c, c, origin),
            cut(hid, c, c, origin),
            sems.at[c, origin],
            recv_h.at[c, origin],
            dev(to, r, m),
        )

    up, down = (g + 1) % G, (g + G - 1) % G

    def goes_up(c):
        return g < (G - 2 if c in shared else G - 1)

    def goes_down(c):
        return g > (1 if c in shared else 0)

    def pass_on(c, origin, has_next, to, sems):
        hop(c, origin, to, sems).wait_recv()

        @pl.when(has_next)
        def _():
            hop(c, origin, to, sems).start()

    def receive(c, k):
        from_left = g >= k
        from_right = g + k < G
        if c in shared:
            from_left = jnp.logical_and(from_left, g < G - 1)
            from_right = jnp.logical_and(from_right, g > 0)

        @pl.when(from_left)
        def _():
            pass_on(c, (g + G - k) % G, goes_up(c), up, send_up)

        @pl.when(from_right)
        def _():
            pass_on(c, (g + k) % G, goes_down(c), down, send_dn)

    def part_copy(c, off):
        r_to = (r + off) % R
        return remote(
            cut(part, c, c, r_to),
            cut(arrived, c, c, r),
            send_p.at[c, off],
            recv_p.at[c, r],
            dev(g, r_to, m),
        )

    def part_in(c, off):
        r_from = (r + off) % R
        return remote(
            cut(part, c, c, r_from),
            cut(arrived, c, c, r_from),
            send_p.at[c, off],
            recv_p.at[c, r_from],
            dev(g, r_from, m),
        )

    def swap_e(b):
        return remote(
            cut(give_e, paired[b], b),
            cut(take_e, paired[b], b),
            send_e.at[b],
            recv_e.at[b],
            dev(g, (r + 1) % R, m),
        )

    def final_e(b, to):
        return remote(
            cut(sum_e, paired[b], b),
            cut(from_e, paired[b], b),
            send_f.at[b],
            recv_f.at[b],
            dev(to, r, m),
        )

    def tok_copy(off):
        return remote(
            tok_mine, tok_g.at[g], send_tg.at[off], recv_tg.at[g], dev((g + off) % G, r, m)
        )

    def tok_in(off):
        g_from = (g + off) % G
        return remote(
            tok_mine, tok_g.at[g_from], send_tg.at[off], recv_tg.at[g_from], dev(g_from, r, m)
        )

    def sum_copy(off):
        return remote(
            tok_sum, tok_r.at[r], send_tr.at[off], recv_tr.at[r], dev(g, (r + off) % R, m)
        )

    def sum_in(off):
        r_from = (r + off) % R
        return remote(
            tok_sum, tok_r.at[r_from], send_tr.at[off], recv_tr.at[r_from], dev(g, r_from, m)
        )

    def over_r(body):
        def step(off, carry):
            body(off)
            return carry

        lax.fori_loop(1, R, step, 0)

    small = [
        pltpu.make_async_copy(a, b, load_s.at[i])
        for i, (a, b) in enumerate(
            (
                (flags_hbm, flags_ref),
                (owner_hbm, owner_ref),
                (mult_hbm, mult_ref),
                (pieces_hbm, pieces_ref),
            )
        )
    ]
    for copy in small:
        copy.start()
    load_cot = pltpu.make_async_copy(cot_hbm, cot_ref, load_c)
    load_cot.start()
    for c in range(chunks):
        load(gate_hbm, gate_in, c, load_g).start()
        load(lift_hbm, lift_in, c, load_l).start()

    barrier = pltpu.get_barrier_semaphore()

    def greet(where):
        pl.semaphore_signal(
            barrier, inc=1, device_id=where, device_id_type=pl.DeviceIdType.MESH
        )

    for off in range(1, M):
        greet(dev(g, r, (m + off) % M))
    for off in range(1, G):
        greet(dev((g + off) % G, r, m))
    over_r(lambda off: greet(dev(g, (r + off) % R, m)))

    for copy in small:
        copy.wait()
    flag = flags_ref[0].astype(jnp.float32)
    scales = []
    token_sum = jnp.float32(0)
    row = lax.broadcasted_iota(jnp.int32, (toks, wide), 0)
    for k in range(slots):
        live = pieces_ref[owner_ref[0, k]] * TILE
        weight = flag * mult_ref[0, k].astype(jnp.float32)
        scales.append(jnp.where(row < live, weight, 0.0))
        token_sum = token_sum + weight * live.astype(jnp.float32)
    tok_mine[...] = jnp.full(tok_mine.shape, token_sum, jnp.float32)

    def make_hidden(c):
        load(gate_hbm, gate_in, c, load_g).wait()
        load(lift_hbm, lift_in, c, load_l).wait()
        for k in range(slots):
            rk = pl.ds(k * toks, toks)
            cols = pl.ds(0, widths[c])
            v = gate_in[c, rk, cols].astype(jnp.float32)
            u = lift_in[c, rk, cols].astype(jnp.float32)
            h = v / (1.0 + jnp.exp(-v)) * u * scales[k][:, : widths[c]]
            hid[c, g, rk, cols] = h.astype(jnp.bfloat16)

    if G >= 3:
        up_ways = (
            jnp.logical_and(g >= 1, g < G - 2),
            g == G - 2,
            g == 0,
        )
        down_ways = (
            jnp.logical_and(g > 1, g <= G - 2),
            g == 1,
            g == G - 1,
        )
    else:
        up_ways, down_ways = (g < G - 1,), (g > 0,)
    ways = len(up_ways)
    made = [0]
    sent = [0] * ways

    def send_to(*counts):
        counts = [min(c, chunks) for c in counts[-ways:]]
        for c in range(max(counts)):
            while made[0] <= c:
                make_hidden(made[0])
                made[0] += 1
            for way in range(ways):
                if sent[way] <= c < counts[way] and not (way == 1 and c in shared):

                    @pl.when(up_ways[way])
                    def _():
                        hop(c, g, up, send_up).start()

                    @pl.when(down_ways[way])
                    def _():
                        hop(c, g, down, send_dn).start()

        for way in range(ways):
            sent[way] = max(sent[way], counts[way])

    load_cot.wait()
    quarters[m] = cot_ref[pl.ds(pl.multiple_of(m * quarter, quarter), quarter), :]
    make_hidden(0)
    made[0] = 1
    pl.semaphore_wait(barrier, M - 1 + G - 1 + R - 1)

    for off in range(1, M):
        spread_copy(off).start()
    for off in range(1, G):
        tok_copy(off).start()
    send_to(*EARLY)
    for off in range(1, M):
        spread_in(off).wait_recv()

    def direct(i, body):
        if not shared:
            body(cross_copy(i))
            return
        by_hand = jnp.logical_or(
            jnp.logical_and(i == G - 1, g < G - 2), jnp.logical_and(i == 0, g > 1)
        )

        @pl.when(jnp.logical_not(by_hand))
        def _():
            body(cross_copy(i))

    def direct_x(i, body):
        by_hand = jnp.logical_or(
            jnp.logical_and(i == G - 1, g < G - 2), jnp.logical_and(i == 0, g > 1)
        )

        @pl.when(jnp.logical_not(by_hand))
        def _():
            body(extra_copy(i))

    def passed(i):
        return jnp.logical_and(helper, jnp.logical_and(i != g, i != buddy))

    others(range(G - 1, 0, -1), lambda i: direct(i, lambda copy: copy.start()))
    share_out(cot_all, quarters.at[g], g, send_3, recv_3)
    cot_all[m, g] = quarters[g]
    send_to(*MID)

    def share_cot(reach):
        def one(i):
            cross_in(i).wait_recv()
            if shared:

                @pl.when(passed(i))
                def _():
                    pass_extra(i).start()

            share_out(cot_all, cot_all.at[m, i], i, send_3, recv_3)

        others(reach, one)

    if STAGES[1] < 0:
        share_cot(range(1, 2))
    if shared:
        others(range(G - 1, 0, -1), lambda i: direct_x(i, lambda copy: copy.start()))
    send_to(*NEXT)

    def relay_cot(reach):
        others(reach, lambda i: relay(cot_all, i, send_3, recv_3))

    def turn_cot():
        for i in range(G):
            share_end(cot_all, i, send_3, recv_3)
            block = jnp.concatenate([cot_all[j, i] for j in range(M)], axis=0)
            cot_t[:, pl.ds(i * n, n)] = block.T

    def share_extra():
        share_out(cot_x, quarters.at[buddy], g, send_y, recv_y)
        cot_x[m, g] = quarters[buddy]

        def more(i):
            extra_in(i).wait_recv()

            @pl.when(passed(i))
            def _():
                pass_cot(i).start()

            share_out(cot_x, cot_x.at[m, i], i, send_y, recv_y)

        others(range(1, G), more)

    def relay_extra():
        others(range(G), lambda i: relay(cot_x, i, send_y, recv_y))

    def turn_extra():
        for i in range(G):
            share_end(cot_x, i, send_y, recv_y)
            block = jnp.concatenate([cot_x[j, i] for j in range(M)], axis=0)
            cot_e[:, pl.ds(i * n, n)] = block.T

    def product(left, block):
        return jnp.dot(left, block, preferred_element_type=jnp.float32)

    def strip(ref, which):
        return ref[pl.ds(pl.multiple_of(which * rows, rows), rows), :]

    def main(c, left_ref, block):
        def other(off):
            r_to = (r + off) % R
            cut(part, c, c, r_to)[...] = product(strip(left_ref, r_to), block).astype(
                jnp.bfloat16
            )
            part_copy(c, off).start()

        over_r(other)
        out_ref[:, columns(c)] = product(strip(left_ref, r), block)

    def every(c):
        return hid[c, :, :, pl.ds(0, widths[c])].reshape(G * n, widths[c])

    def doer(c):
        return helper if c in shared else at_edge

    def compute(c):
        if c not in paired:
            main(c, cot_t, every(c))
            return
        b = paired.index(c)

        @pl.when(doer(c))
        def _():
            block = every(c)
            cut(give_e, c, b)[...] = product(strip(cot_e, (r + 1) % R), block).astype(
                jnp.bfloat16
            )
            swap_e(b).start()
            main(c, cot_t, block)
            cut(mine_e, c, b)[...] = product(strip(cot_e, r), block)

    def hand_over(c):
        b = paired.index(c)

        @pl.when(doer(c))
        def _():
            swap_e(b).wait_recv()
            total = cut(mine_e, c, b)[...] + cut(take_e, c, b)[...].astype(jnp.float32)
            cut(sum_e, c, b)[...] = total.astype(jnp.bfloat16)
            final_e(b, buddy).start()

    def tokens_g():
        total = tok_mine[...]
        for off in range(1, G):
            tok_in(off).wait_recv()
            total = total + tok_g[(g + off) % G]
        tok_sum[...] = total
        over_r(lambda off: sum_copy(off).start())

    def add_tokens(off, total):
        sum_in(off).wait_recv()
        return total + tok_r[(r + off) % R]

    inverse = []

    def finish(c):
        cols = columns(c)
        if not inverse:
            total = lax.fori_loop(1, R, add_tokens, tok_sum[...])
            inverse.append((1.0 / total)[0:1, 0:1])

        def add_part(off):
            part_in(c, off).wait_recv()
            out_ref[:, cols] = out_ref[:, cols] + cut(arrived, c, c, (r + off) % R)[
                ...
            ].astype(jnp.float32)

        if c not in paired:
            over_r(add_part)
            out_ref[:, cols] = out_ref[:, cols] * inverse[0]
            return

        @pl.when(doer(c))
        def _():
            over_r(add_part)
            out_ref[:, cols] = out_ref[:, cols] * inverse[0]

        @pl.when(jnp.logical_not(doer(c)))
        def _():
            b = paired.index(c)
            final_e(b, buddy).wait_recv()
            out_ref[:, cols] = cut(from_e, c, b)[...].astype(jnp.float32) * inverse[0]

    near, away = range(1, 2), range(2, G)
    steps = [
        (STAGES[0], lambda: relay_cot(range(1))),
        (STAGES[1], lambda: share_cot(near)),
        (STAGES[2], lambda: share_cot(away)),
        (STAGES[3], lambda: relay_cot(near)),
        (STAGES[4], lambda: relay_cot(away)),
        (STAGES[5], turn_cot),
    ]
    if shared:
        steps.insert(3, (EXTRA[0], share_extra))
        steps.insert(6, (EXTRA[1], relay_extra))
        steps.append((EXTRA[2], turn_extra))
    done = []
    ready = 0
    handed = 0
    start = {}
    for t in range(chunks + 1):
        if t < chunks:
            receive(t, 1)
        send_to(*(t + 1 + ahead for ahead in AHEAD))
        for half in range(2):
            if half and t >= 1:
                for k in range(2, G):
                    receive(t - 1, k)
            for at, step in steps:
                if at == 2 * t + half:
                    step()
            if 2 * t + half == TOKENS:
                tokens_g()
        turned = 2 * t + 1 >= STAGES[5]
        turned_e = 2 * t + 1 >= EXTRA[2]
        while turned and ready < t and (turned_e or ready not in paired):
            compute(ready)
            start[ready] = t
            ready += 1
        while handed < ready and t >= start[handed] + HAND:
            if handed in paired:
                hand_over(handed)
            handed += 1
        if turned and t >= STAGES[5] // 2 + LAG:
            for c in range(min(t - 1 - LAG, ready)):
                if c not in done and c not in paired:
                    finish(c)
                    done.append(c)
    for c in range(handed, chunks):
        if c in paired:
            hand_over(c)
    for c in range(chunks):
        if c not in done:
            finish(c)

    for off in range(1, M):
        spread_copy(off).wait_send()
    for off in range(1, G):
        tok_copy(off).wait_send()
    others(range(1, G), lambda i: direct(i, lambda copy: copy.wait_send()))
    for i in range(G):
        share_drain(cot_all, i, send_3, recv_3)
    if shared:
        others(range(1, G), lambda i: direct_x(i, lambda copy: copy.wait_send()))
        for i in range(G):
            share_drain(cot_x, i, send_y, recv_y)

            @pl.when(passed(i))
            def _():
                pass_cot(i).wait_send()
                pass_extra(i).wait_send()

        for b, c in enumerate(paired):

            @pl.when(doer(c))
            def _():
                swap_e(b).wait_send()
                final_e(b, buddy).wait_send()

    for c in range(chunks):
        for i in range(G):

            @pl.when(jnp.logical_and(i <= g, goes_up(c)))
            def _():
                hop(c, i, up, send_up).wait_send()

            @pl.when(jnp.logical_and(i >= g, goes_down(c)))
            def _():
                hop(c, i, down, send_dn).wait_send()

    def drain(off):
        sum_copy(off).wait_send()
        for c in range(chunks):
            if c not in paired:
                part_copy(c, off).wait_send()
                continue

            @pl.when(doer(c))
            def _():
                part_copy(c, off).wait_send()

    over_r(drain)


def on_device(
    mesh_shape,
    gating_logits,
    lifted_hidden_values,
    loss_output_grad,
    arrival_flags,
    block_owner_map,
    decoder_multipliers,
    block_piece_number,
):
    dp, M = mesh_shape
    G = M
    R = dp // G
    _, slots, toks, width = gating_logits.shape
    feats = loss_output_grad.shape[3]
    rows = feats * M // dp
    widths = chunk_widths(width)
    chunks = len(widths)
    wide = max(widths)
    n = slots * toks
    shared = SHARED if R == 2 and G == 4 else ()
    returned = RETURNED if R == 2 and G == 4 else ()
    sizes = (G, R, M, slots, toks, widths, rows, shared, returned)
    nb = max(len(shared) + len(returned), 1)
    far = G if shared else 1
    vmem = pl.BlockSpec(memory_space=pltpu.VMEM)
    dma = pltpu.SemaphoreType.DMA
    bf, f32 = jnp.bfloat16, jnp.float32
    return pl.pallas_call(
        functools.partial(kernel, sizes),
        out_shape=pltpu.VMEM((rows, width), f32),
        in_specs=[pl.BlockSpec(memory_space=pl.ANY)] * 7,
        out_specs=vmem,
        scratch_shapes=[
            pltpu.VMEM((chunks, n, wide), bf),
            pltpu.VMEM((chunks, n, wide), bf),
            pltpu.VMEM((n, feats), bf),
            pltpu.VMEM((M, n // M, feats), bf),
            pltpu.VMEM((chunks, G, n, wide), bf),
            pltpu.VMEM((M, G, n // M, feats), bf),
            pltpu.VMEM((feats, G * n), bf),
            pltpu.VMEM((chunks, R, rows, wide), bf),
            pltpu.VMEM((chunks, R, rows, wide), bf),
            pltpu.VMEM((8, 128), f32),
            pltpu.VMEM((G, 8, 128), f32),
            pltpu.VMEM((8, 128), f32),
            pltpu.VMEM((R, 8, 128), f32),
            pltpu.VMEM((M, far, n // M, feats), bf),
            pltpu.VMEM((feats, G * n), bf),
            pltpu.VMEM((nb, rows, wide), f32),
            pltpu.VMEM((nb, rows, wide), bf),
            pltpu.VMEM((nb, rows, wide), bf),
            pltpu.VMEM((nb, rows, wide), bf),
            pltpu.VMEM((nb, rows, wide), bf),
            dma,
            dma((chunks,)),
            dma((chunks,)),
            dma((M,)),
            dma((M,)),
            dma((G,)),
            dma((G,)),
            dma((M, G)),
            dma((M, G)),
            dma((chunks, G)),
            dma((chunks, G)),
            dma((chunks, G)),
            dma((chunks, R)),
            dma((chunks, R)),
            dma((G,)),
            dma((G,)),
            dma((R,)),
            dma((R,)),
            dma((G,)),
            dma((G,)),
            dma((M, G)),
            dma((M, G)),
            dma((nb,)),
            dma((nb,)),
            dma((nb,)),
            dma((nb,)),
            dma((G,)),
            dma((G,)),
            pltpu.SMEM(arrival_flags.shape, jnp.int32),
            pltpu.SMEM(block_owner_map.shape, jnp.int32),
            pltpu.SMEM(decoder_multipliers.shape, jnp.int32),
            pltpu.SMEM(block_piece_number.shape, jnp.int32),
            dma((4,)),
        ],
        compiler_params=pltpu.CompilerParams(
            collective_id=0, has_side_effects=True, vmem_limit_bytes=58_000_000
        ),
    )(
        arrival_flags,
        block_owner_map,
        decoder_multipliers,
        block_piece_number,
        gating_logits.reshape(n, width),
        lifted_hidden_values.reshape(n, width),
        loss_output_grad.reshape(n, feats),
    )


def solution(mesh):
    shape = (mesh.shape["dp"], mesh.shape["mp"])
    return jax.shard_map(
        functools.partial(on_device, shape),
        mesh=mesh,
        in_specs=(
            P("dp", None, None, "mp"),
            P("dp", None, None, "mp"),
            P("dp", None, None, "mp"),
            P("dp"),
            P("dp", None),
            P("dp", None),
            P(),
        ),
        out_specs=P("dp", "mp"),
        check_vma=False,
    )
```

```python
import functools

import jax
import jax.numpy as jnp
from jax import lax
from jax.experimental import pallas as pl
from jax.experimental.pallas import tpu as pltpu
from jax.sharding import PartitionSpec as P

TILE = 32
CHUNK = 256
LANES = 128
HEAD = 2
TAIL = 4
SHARED = (2, 4, 6, 7, 8)
RETURNED = (3, 5)
AHEAD = (2, 9, 8)
EARLY = (3, 4, 2)
MID = (2, 6, 2)
NEXT = (1, 2, 1)
STAGES = (2, 0, 2, 3, 4, 4)
EXTRA = (2, 7, 7)
LAG = 5
HAND = 2
TOKENS = 4


def chunk_widths(width):
    full, rest = divmod(width - LANES * (HEAD + TAIL), CHUNK)
    return (LANES,) * HEAD + (CHUNK,) * full + (LANES,) * (TAIL + rest // LANES)


def kernel(
    sizes,
    flags_hbm,
    owner_hbm,
    mult_hbm,
    pieces_hbm,
    gate_hbm,
    lift_hbm,
    cot_hbm,
    out_ref,
    gate_in,
    lift_in,
    cot_ref,
    quarters,
    hid,
    cot_all,
    cot_t,
    part,
    arrived,
    tok_mine,
    tok_g,
    tok_sum,
    tok_r,
    cot_x,
    cot_e,
    mine_e,
    give_e,
    take_e,
    sum_e,
    from_e,
    load_c,
    load_g,
    load_l,
    send_1,
    recv_1,
    send_2,
    recv_2,
    send_3,
    recv_3,
    send_up,
    send_dn,
    recv_h,
    send_p,
    recv_p,
    send_tg,
    recv_tg,
    send_tr,
    recv_tr,
    send_x,
    recv_x,
    send_y,
    recv_y,
    send_e,
    recv_e,
    send_f,
    recv_f,
    send_r,
    send_s,
    flags_ref,
    owner_ref,
    mult_ref,
    pieces_ref,
    load_s,
):
    G, R, M, slots, toks, widths, rows, shared, returned = sizes
    chunks = len(widths)
    starts = [sum(widths[:c]) for c in range(chunks)]
    wide = max(widths)
    n = slots * toks
    d = lax.axis_index("dp")
    m = lax.axis_index("mp")
    g = d // R
    r = d % R
    quarter = n // M
    pair = M == 4
    m1 = m + 1 - 2 * (m % 2)
    m2 = m + 2 - 4 * (m // 2)
    m3 = m1 + 2 - 4 * (m1 // 2)

    at_edge = jnp.logical_or(g == 0, g == G - 1)
    helper = jnp.logical_not(at_edge)
    buddy = g + 1 - 2 * (g % 2)
    paired = shared + returned

    def dev(g_to, r_to, m_to):
        return {"dp": g_to * R + r_to, "mp": m_to}

    def remote(src, dst, s, q, where):
        return pltpu.make_async_remote_copy(
            src_ref=src,
            dst_ref=dst,
            send_sem=s,
            recv_sem=q,
            device_id=where,
            device_id_type=pl.DeviceIdType.MESH,
        )

    def spread_copy(off):
        m_to = (m + off) % M
        return remote(
            cot_ref.at[pl.ds(pl.multiple_of(m_to * quarter, quarter), quarter)],
            quarters.at[m],
            send_1.at[off],
            recv_1.at[m],
            dev(g, r, m_to),
        )

    def spread_in(off):
        m_from = (m + off) % M
        return remote(
            quarters.at[m_from],
            quarters.at[m_from],
            send_1.at[off],
            recv_1.at[m_from],
            dev(g, r, m_from),
        )

    def cross_copy(g_to):
        return remote(
            quarters.at[g_to], cot_all.at[m, g], send_2.at[g_to], recv_2.at[g], dev(g_to, r, m)
        )

    def cross_in(g_from):
        return remote(
            quarters.at[g],
            cot_all.at[m, g_from],
            send_2.at[g_from],
            recv_2.at[g_from],
            dev(g_from, r, m),
        )

    def extra_copy(g_to):
        return remote(
            quarters.at[g_to + 1 - 2 * (g_to % 2)],
            cot_x.at[m, g],
            send_x.at[g_to],
            recv_x.at[g],
            dev(g_to, r, m),
        )

    def pass_cot(g_from):
        return remote(
            cot_x.at[m, g_from],
            cot_all.at[m, g_from],
            send_r.at[g_from],
            recv_2.at[g_from],
            dev(buddy, r, m),
        )

    def pass_extra(g_from):
        return remote(
            cot_all.at[m, g_from],
            cot_x.at[m, g_from],
            send_s.at[g_from],
            recv_x.at[g_from],
            dev(buddy, r, m),
        )

    def extra_in(g_from):
        return remote(
            quarters.at[0], cot_x.at[m, g_from], send_x.at[0], recv_x.at[g_from], dev(g_from, r, m)
        )

    def share(src, buf, origin, i, way, to, sends, recvs):
        return remote(
            src, buf.at[origin, i], sends.at[way, i], recvs.at[origin, i], dev(g, r, to)
        )

    peers = [m1, m2] if pair else [(m + off) % M for off in range(1, M)]

    def share_out(buf, src, i, sends, recvs):
        for way, to in enumerate(peers):
            share(src, buf, m, i, way, to, sends, recvs).start()

    def relay(buf, i, sends, recvs):
        if pair:
            share(buf.at[m2, i], buf, m2, i, 2, m1, sends, recvs).wait_recv()
            share(buf.at[m2, i], buf, m2, i, 2, m1, sends, recvs).start()

    def share_end(buf, i, sends, recvs):
        for o in [m1, m3] if pair else peers:
            share(buf.at[o, i], buf, o, i, 0, m1, sends, recvs).wait_recv()

    def share_drain(buf, i, sends, recvs):
        for way, to in enumerate(peers):
            share(buf.at[m, i], buf, m, i, way, to, sends, recvs).wait_send()
        if pair:
            share(buf.at[m2, i], buf, m2, i, 2, m1, sends, recvs).wait_send()

    def others(reach, body):
        for k in reach:
            if k == 0:
                body(g)
                continue

            @pl.when(g >= k)
            def _():
                body(g - k)

            @pl.when(g + k < G)
            def _():
                body(g + k)

    def cut(ref, c, *index):
        if widths[c] == wide:
            return ref.at[index]
        return ref.at[(*index, slice(None), pl.ds(0, widths[c]))]

    def columns(c):
        return pl.ds(starts[c], widths[c])

    def load(src, dst, c, sem):
        return pltpu.make_async_copy(
            src.at[:, columns(c)], cut(dst, c, c), sem.at[c]
        )

    def hop(c, origin, to, sems):
        return remote(
            cut(hid, c, c, origin),
            cut(hid, c, c, origin),
            sems.at[c, origin],
            recv_h.at[c, origin],
            dev(to, r, m),
        )

    up, down = (g + 1) % G, (g + G - 1) % G

    def goes_up(c):
        return g < (G - 2 if c in shared else G - 1)

    def goes_down(c):
        return g > (1 if c in shared else 0)

    def pass_on(c, origin, has_next, to, sems):
        hop(c, origin, to, sems).wait_recv()

        @pl.when(has_next)
        def _():
            hop(c, origin, to, sems).start()

    def receive(c, k):
        from_left = g >= k
        from_right = g + k < G
        if c in shared:
            from_left = jnp.logical_and(from_left, g < G - 1)
            from_right = jnp.logical_and(from_right, g > 0)

        @pl.when(from_left)
        def _():
            pass_on(c, (g + G - k) % G, goes_up(c), up, send_up)

        @pl.when(from_right)
        def _():
            pass_on(c, (g + k) % G, goes_down(c), down, send_dn)

    def part_copy(c, off):
        r_to = (r + off) % R
        return remote(
            cut(part, c, c, r_to),
            cut(arrived, c, c, r),
            send_p.at[c, off],
            recv_p.at[c, r],
            dev(g, r_to, m),
        )

    def part_in(c, off):
        r_from = (r + off) % R
        return remote(
            cut(part, c, c, r_from),
            cut(arrived, c, c, r_from),
            send_p.at[c, off],
            recv_p.at[c, r_from],
            dev(g, r_from, m),
        )

    def swap_e(b):
        return remote(
            cut(give_e, paired[b], b),
            cut(take_e, paired[b], b),
            send_e.at[b],
            recv_e.at[b],
            dev(g, (r + 1) % R, m),
        )

    def final_e(b, to):
        return remote(
            cut(sum_e, paired[b], b),
            cut(from_e, paired[b], b),
            send_f.at[b],
            recv_f.at[b],
            dev(to, r, m),
        )

    def tok_copy(off):
        return remote(
            tok_mine, tok_g.at[g], send_tg.at[off], recv_tg.at[g], dev((g + off) % G, r, m)
        )

    def tok_in(off):
        g_from = (g + off) % G
        return remote(
            tok_mine, tok_g.at[g_from], send_tg.at[off], recv_tg.at[g_from], dev(g_from, r, m)
        )

    def sum_copy(off):
        return remote(
            tok_sum, tok_r.at[r], send_tr.at[off], recv_tr.at[r], dev(g, (r + off) % R, m)
        )

    def sum_in(off):
        r_from = (r + off) % R
        return remote(
            tok_sum, tok_r.at[r_from], send_tr.at[off], recv_tr.at[r_from], dev(g, r_from, m)
        )

    def over_r(body):
        def step(off, carry):
            body(off)
            return carry

        lax.fori_loop(1, R, step, 0)

    small = [
        pltpu.make_async_copy(a, b, load_s.at[i])
        for i, (a, b) in enumerate(
            (
                (flags_hbm, flags_ref),
                (owner_hbm, owner_ref),
                (mult_hbm, mult_ref),
                (pieces_hbm, pieces_ref),
            )
        )
    ]
    for copy in small:
        copy.start()
    load_cot = pltpu.make_async_copy(cot_hbm, cot_ref, load_c)
    load_cot.start()
    for c in range(chunks):
        load(gate_hbm, gate_in, c, load_g).start()
        load(lift_hbm, lift_in, c, load_l).start()

    barrier = pltpu.get_barrier_semaphore()

    def greet(where):
        pl.semaphore_signal(
            barrier, inc=1, device_id=where, device_id_type=pl.DeviceIdType.MESH
        )

    for off in range(1, M):
        greet(dev(g, r, (m + off) % M))
    for off in range(1, G):
        greet(dev((g + off) % G, r, m))
    over_r(lambda off: greet(dev(g, (r + off) % R, m)))

    for copy in small:
        copy.wait()
    flag = flags_ref[0].astype(jnp.float32)
    scales = []
    token_sum = jnp.float32(0)
    row = lax.broadcasted_iota(jnp.int32, (toks, wide), 0)
    for k in range(slots):
        live = pieces_ref[owner_ref[0, k]] * TILE
        weight = flag * mult_ref[0, k].astype(jnp.float32)
        scales.append(jnp.where(row < live, weight, 0.0))
        token_sum = token_sum + weight * live.astype(jnp.float32)
    tok_mine[...] = jnp.full(tok_mine.shape, token_sum, jnp.float32)

    def make_hidden(c):
        load(gate_hbm, gate_in, c, load_g).wait()
        load(lift_hbm, lift_in, c, load_l).wait()
        for k in range(slots):
            rk = pl.ds(k * toks, toks)
            cols = pl.ds(0, widths[c])
            v = gate_in[c, rk, cols].astype(jnp.float32)
            u = lift_in[c, rk, cols].astype(jnp.float32)
            h = v / (1.0 + jnp.exp(-v)) * u * scales[k][:, : widths[c]]
            hid[c, g, rk, cols] = h.astype(jnp.bfloat16)

    if G >= 3:
        up_ways = (
            jnp.logical_and(g >= 1, g < G - 2),
            g == G - 2,
            g == 0,
        )
        down_ways = (
            jnp.logical_and(g > 1, g <= G - 2),
            g == 1,
            g == G - 1,
        )
    else:
        up_ways, down_ways = (g < G - 1,), (g > 0,)
    ways = len(up_ways)
    made = [0]
    sent = [0] * ways

    def send_to(*counts):
        counts = [min(c, chunks) for c in counts[-ways:]]
        for c in range(max(counts)):
            while made[0] <= c:
                make_hidden(made[0])
                made[0] += 1
            for way in range(ways):
                if sent[way] <= c < counts[way] and not (way == 1 and c in shared):

                    @pl.when(up_ways[way])
                    def _():
                        hop(c, g, up, send_up).start()

                    @pl.when(down_ways[way])
                    def _():
                        hop(c, g, down, send_dn).start()

        for way in range(ways):
            sent[way] = max(sent[way], counts[way])

    load_cot.wait()
    quarters[m] = cot_ref[pl.ds(pl.multiple_of(m * quarter, quarter), quarter), :]
    make_hidden(0)
    made[0] = 1
    pl.semaphore_wait(barrier, M - 1 + G - 1 + R - 1)

    for off in range(1, M):
        spread_copy(off).start()
    for off in range(1, G):
        tok_copy(off).start()
    send_to(*EARLY)
    for off in range(1, M):
        spread_in(off).wait_recv()

    def direct(i, body):
        if not shared:
            body(cross_copy(i))
            return
        by_hand = jnp.logical_or(
            jnp.logical_and(i == G - 1, g < G - 2), jnp.logical_and(i == 0, g > 1)
        )

        @pl.when(jnp.logical_not(by_hand))
        def _():
            body(cross_copy(i))

    def direct_x(i, body):
        by_hand = jnp.logical_or(
            jnp.logical_and(i == G - 1, g < G - 2), jnp.logical_and(i == 0, g > 1)
        )

        @pl.when(jnp.logical_not(by_hand))
        def _():
            body(extra_copy(i))

    def passed(i):
        return jnp.logical_and(helper, jnp.logical_and(i != g, i != buddy))

    others(range(G - 1, 0, -1), lambda i: direct(i, lambda copy: copy.start()))
    share_out(cot_all, quarters.at[g], g, send_3, recv_3)
    cot_all[m, g] = quarters[g]
    send_to(*MID)

    def share_cot(reach):
        def one(i):
            cross_in(i).wait_recv()
            if shared:

                @pl.when(passed(i))
                def _():
                    pass_extra(i).start()

            share_out(cot_all, cot_all.at[m, i], i, send_3, recv_3)

        others(reach, one)

    if STAGES[1] < 0:
        share_cot(range(1, 2))
    if shared:
        others(range(G - 1, 0, -1), lambda i: direct_x(i, lambda copy: copy.start()))
    send_to(*NEXT)

    def relay_cot(reach):
        others(reach, lambda i: relay(cot_all, i, send_3, recv_3))

    def turn_cot():
        for i in range(G):
            share_end(cot_all, i, send_3, recv_3)
            block = jnp.concatenate([cot_all[j, i] for j in range(M)], axis=0)
            cot_t[:, pl.ds(i * n, n)] = block.T

    def share_extra():
        share_out(cot_x, quarters.at[buddy], g, send_y, recv_y)
        cot_x[m, g] = quarters[buddy]

        def more(i):
            extra_in(i).wait_recv()

            @pl.when(passed(i))
            def _():
                pass_cot(i).start()

            share_out(cot_x, cot_x.at[m, i], i, send_y, recv_y)

        others(range(1, G), more)

    def relay_extra():
        others(range(G), lambda i: relay(cot_x, i, send_y, recv_y))

    def turn_extra():
        for i in range(G):
            share_end(cot_x, i, send_y, recv_y)
            block = jnp.concatenate([cot_x[j, i] for j in range(M)], axis=0)
            cot_e[:, pl.ds(i * n, n)] = block.T

    def product(left, block):
        return jnp.dot(left, block, preferred_element_type=jnp.float32)

    def strip(ref, which):
        return ref[pl.ds(pl.multiple_of(which * rows, rows), rows), :]

    def main(c, left_ref, block):
        def other(off):
            r_to = (r + off) % R
            cut(part, c, c, r_to)[...] = product(strip(left_ref, r_to), block).astype(
                jnp.bfloat16
            )
            part_copy(c, off).start()

        over_r(other)
        out_ref[:, columns(c)] = product(strip(left_ref, r), block)

    def every(c):
        return hid[c, :, :, pl.ds(0, widths[c])].reshape(G * n, widths[c])

    def doer(c):
        return helper if c in shared else at_edge

    def compute(c):
        if c not in paired:
            main(c, cot_t, every(c))
            return
        b = paired.index(c)

        @pl.when(doer(c))
        def _():
            block = every(c)
            cut(give_e, c, b)[...] = product(strip(cot_e, (r + 1) % R), block).astype(
                jnp.bfloat16
            )
            swap_e(b).start()
            main(c, cot_t, block)
            cut(mine_e, c, b)[...] = product(strip(cot_e, r), block)

    def hand_over(c):
        b = paired.index(c)

        @pl.when(doer(c))
        def _():
            swap_e(b).wait_recv()
            total = cut(mine_e, c, b)[...] + cut(take_e, c, b)[...].astype(jnp.float32)
            cut(sum_e, c, b)[...] = total.astype(jnp.bfloat16)
            final_e(b, buddy).start()

    def tokens_g():
        total = tok_mine[...]
        for off in range(1, G):
            tok_in(off).wait_recv()
            total = total + tok_g[(g + off) % G]
        tok_sum[...] = total
        over_r(lambda off: sum_copy(off).start())

    def add_tokens(off, total):
        sum_in(off).wait_recv()
        return total + tok_r[(r + off) % R]

    inverse = []

    def finish(c):
        cols = columns(c)
        if not inverse:
            total = lax.fori_loop(1, R, add_tokens, tok_sum[...])
            inverse.append((1.0 / total)[0:1, 0:1])

        def add_part(off):
            part_in(c, off).wait_recv()
            out_ref[:, cols] = out_ref[:, cols] + cut(arrived, c, c, (r + off) % R)[
                ...
            ].astype(jnp.float32)

        if c not in paired:
            over_r(add_part)
            out_ref[:, cols] = out_ref[:, cols] * inverse[0]
            return

        @pl.when(doer(c))
        def _():
            over_r(add_part)
            out_ref[:, cols] = out_ref[:, cols] * inverse[0]

        @pl.when(jnp.logical_not(doer(c)))
        def _():
            b = paired.index(c)
            final_e(b, buddy).wait_recv()
            out_ref[:, cols] = cut(from_e, c, b)[...].astype(jnp.float32) * inverse[0]

    near, away = range(1, 2), range(2, G)
    steps = [
        (STAGES[0], lambda: relay_cot(range(1))),
        (STAGES[1], lambda: share_cot(near)),
        (STAGES[2], lambda: share_cot(away)),
        (STAGES[3], lambda: relay_cot(near)),
        (STAGES[4], lambda: relay_cot(away)),
        (STAGES[5], turn_cot),
    ]
    if shared:
        steps.insert(3, (EXTRA[0], share_extra))
        steps.insert(6, (EXTRA[1], relay_extra))
        steps.append((EXTRA[2], turn_extra))
    done = []
    ready = 0
    handed = 0
    start = {}
    for t in range(chunks + 1):
        if t < chunks:
            receive(t, 1)
        send_to(*(t + 1 + ahead for ahead in AHEAD))
        for half in range(2):
            if half and t >= 1:
                for k in range(2, G):
                    receive(t - 1, k)
            for at, step in steps:
                if at == 2 * t + half:
                    step()
            if 2 * t + half == TOKENS:
                tokens_g()
        turned = 2 * t + 1 >= STAGES[5]
        turned_e = 2 * t + 1 >= EXTRA[2]
        while turned and ready < t and (turned_e or ready not in paired):
            compute(ready)
            start[ready] = t
            ready += 1
        while handed < ready and t >= start[handed] + HAND:
            if handed in paired:
                hand_over(handed)
            handed += 1
        if turned and t >= STAGES[5] // 2 + LAG:
            for c in range(min(t - 1 - LAG, ready)):
                if c not in done and (c not in paired or t >= start[c] + HAND + 4):
                    finish(c)
                    done.append(c)
    for c in range(handed, chunks):
        if c in paired:
            hand_over(c)
    for c in range(chunks):
        if c not in done:
            finish(c)

    for off in range(1, M):
        spread_copy(off).wait_send()
    for off in range(1, G):
        tok_copy(off).wait_send()
    others(range(1, G), lambda i: direct(i, lambda copy: copy.wait_send()))
    for i in range(G):
        share_drain(cot_all, i, send_3, recv_3)
    if shared:
        others(range(1, G), lambda i: direct_x(i, lambda copy: copy.wait_send()))
        for i in range(G):
            share_drain(cot_x, i, send_y, recv_y)

            @pl.when(passed(i))
            def _():
                pass_cot(i).wait_send()
                pass_extra(i).wait_send()

        for b, c in enumerate(paired):

            @pl.when(doer(c))
            def _():
                swap_e(b).wait_send()
                final_e(b, buddy).wait_send()

    for c in range(chunks):
        for i in range(G):

            @pl.when(jnp.logical_and(i <= g, goes_up(c)))
            def _():
                hop(c, i, up, send_up).wait_send()

            @pl.when(jnp.logical_and(i >= g, goes_down(c)))
            def _():
                hop(c, i, down, send_dn).wait_send()

    def drain(off):
        sum_copy(off).wait_send()
        for c in range(chunks):
            if c not in paired:
                part_copy(c, off).wait_send()
                continue

            @pl.when(doer(c))
            def _():
                part_copy(c, off).wait_send()

    over_r(drain)


def on_device(
    mesh_shape,
    gating_logits,
    lifted_hidden_values,
    loss_output_grad,
    arrival_flags,
    block_owner_map,
    decoder_multipliers,
    block_piece_number,
):
    dp, M = mesh_shape
    G = M
    R = dp // G
    _, slots, toks, width = gating_logits.shape
    feats = loss_output_grad.shape[3]
    rows = feats * M // dp
    widths = chunk_widths(width)
    chunks = len(widths)
    wide = max(widths)
    n = slots * toks
    shared = SHARED if R == 2 and G == 4 else ()
    returned = RETURNED if R == 2 and G == 4 else ()
    sizes = (G, R, M, slots, toks, widths, rows, shared, returned)
    nb = max(len(shared) + len(returned), 1)
    far = G if shared else 1
    vmem = pl.BlockSpec(memory_space=pltpu.VMEM)
    dma = pltpu.SemaphoreType.DMA
    bf, f32 = jnp.bfloat16, jnp.float32
    return pl.pallas_call(
        functools.partial(kernel, sizes),
        out_shape=pltpu.VMEM((rows, width), f32),
        in_specs=[pl.BlockSpec(memory_space=pl.ANY)] * 7,
        out_specs=vmem,
        scratch_shapes=[
            pltpu.VMEM((chunks, n, wide), bf),
            pltpu.VMEM((chunks, n, wide), bf),
            pltpu.VMEM((n, feats), bf),
            pltpu.VMEM((M, n // M, feats), bf),
            pltpu.VMEM((chunks, G, n, wide), bf),
            pltpu.VMEM((M, G, n // M, feats), bf),
            pltpu.VMEM((feats, G * n), bf),
            pltpu.VMEM((chunks, R, rows, wide), bf),
            pltpu.VMEM((chunks, R, rows, wide), bf),
            pltpu.VMEM((8, 128), f32),
            pltpu.VMEM((G, 8, 128), f32),
            pltpu.VMEM((8, 128), f32),
            pltpu.VMEM((R, 8, 128), f32),
            pltpu.VMEM((M, far, n // M, feats), bf),
            pltpu.VMEM((feats, G * n), bf),
            pltpu.VMEM((nb, rows, wide), f32),
            pltpu.VMEM((nb, rows, wide), bf),
            pltpu.VMEM((nb, rows, wide), bf),
            pltpu.VMEM((nb, rows, wide), bf),
            pltpu.VMEM((nb, rows, wide), bf),
            dma,
            dma((chunks,)),
            dma((chunks,)),
            dma((M,)),
            dma((M,)),
            dma((G,)),
            dma((G,)),
            dma((M, G)),
            dma((M, G)),
            dma((chunks, G)),
            dma((chunks, G)),
            dma((chunks, G)),
            dma((chunks, R)),
            dma((chunks, R)),
            dma((G,)),
            dma((G,)),
            dma((R,)),
            dma((R,)),
            dma((G,)),
            dma((G,)),
            dma((M, G)),
            dma((M, G)),
            dma((nb,)),
            dma((nb,)),
            dma((nb,)),
            dma((nb,)),
            dma((G,)),
            dma((G,)),
            pltpu.SMEM(arrival_flags.shape, jnp.int32),
            pltpu.SMEM(block_owner_map.shape, jnp.int32),
            pltpu.SMEM(decoder_multipliers.shape, jnp.int32),
            pltpu.SMEM(block_piece_number.shape, jnp.int32),
            dma((4,)),
        ],
        compiler_params=pltpu.CompilerParams(
            collective_id=0, has_side_effects=True, vmem_limit_bytes=58_000_000
        ),
    )(
        arrival_flags,
        block_owner_map,
        decoder_multipliers,
        block_piece_number,
        gating_logits.reshape(n, width),
        lifted_hidden_values.reshape(n, width),
        loss_output_grad.reshape(n, feats),
    )


def solution(mesh):
    shape = (mesh.shape["dp"], mesh.shape["mp"])
    return jax.shard_map(
        functools.partial(on_device, shape),
        mesh=mesh,
        in_specs=(
            P("dp", None, None, "mp"),
            P("dp", None, None, "mp"),
            P("dp", None, None, "mp"),
            P("dp"),
            P("dp", None),
            P("dp", None),
            P(),
        ),
        out_specs=P("dp", "mp"),
        check_vma=False,
    )
```
